768 devices in a mesh: slab: 768 (over y, z, x, core).
Axes of the slice: x: 4, y: 8, z: 12, core: 2. Of those that a mesh axis runs over, the one named last changes fastest.
Arguments:
- load_terms: float32 [8, 8, 8, 98304], P(None, None, None, 'slab'), may hold values from -12 to 12
- geometry: float32 [3, 8, 8, 8, 98304], P(None, None, None, None, 'slab'), may hold values from 0.02 to 0.2
- mass_terms: float32 [8, 8, 8, 98304], P(None, None, None, 'slab'), may hold values from 1 to 4
- element_order: int32 [768, 128], P('slab'), may hold values from 0 to 127, each once within a row
Outputs:
- solution: float32 [8, 8, 8, 98304], P(None, None, None, 'slab')
- residual: float32 [8, 8, 8, 98304], P(None, None, None, 'slab')
The draws below stay inside these ranges and needn't reach their ends.
Inputs may be any that keep to these rules, and one draw needn't show every extreme that they name: `element_order`: each device's row lists each of its 128 cells once.
All inputs are finite; a program needn't handle non-finite values.
Results may differ from the reference program's by a relative error of at most 0.0001.
Values sent between devices are 32-bit elements; how exact they have to be, the bound alone decides.
No kernel may reach another device: no remote copies, remote signals or barrier semaphores. Data moves between devices by JAX's collectives and lax.ppermute only.
A program may use at most 32 MiB of HBM per device.

```python
import math
import jax
import jax.numpy as jnp
import numpy as np
from jax import lax

POINTS = 8
EL_X = 1
EL_Y = 8
EL_Z = 16
SECTIONS = 2
ELEM_DEV = 128
NELEM = 98304
N_SLAB = 768


def draw_load_terms(key, part):
    noise = jax.random.normal(key, (POINTS, POINTS, POINTS, NELEM), jnp.float32)
    device_pos = (jnp.arange(NELEM) // ELEM_DEV).astype(jnp.float32)
    ramp = 1.0 + 0.8 * device_pos / max(NELEM // ELEM_DEV - 1, 1)
    return jnp.clip(noise * ramp, -12.0, 12.0)


def level_of(own_key, dims, split, smallest, high):
    level = 1.0
    for position, shards_of in split:
        steps = jax.random.uniform(jax.random.fold_in(jax.random.fold_in(own_key, 6), position), (shards_of,), jnp.float32, smallest / len(split), high / len(split))
        level = level * jnp.repeat(jnp.exp(steps), dims[position] // shards_of).reshape((-1,) + (1,) * (len(dims) - 1 - position))
    return level


def setup_inputs(seed: int = 0) -> dict:
    key_of = jax.random.split(jax.random.key(seed), 5)
    load_terms = draw_load_terms(jax.random.fold_in(key_of[4], 71), 0)
    geometry = jnp.clip(jnp.exp(math.log(0.2) - 2.3025851 * jax.random.uniform(key_of[1], (3, POINTS, POINTS, POINTS, NELEM), jnp.float32) ** level_of(key_of[1], (3, POINTS, POINTS, POINTS, NELEM), ((4, 768),), -0.2, 0.2)), 0.02, 0.2)
    mass_terms = jnp.clip(jnp.exp(math.log(4.0) - 1.3862944 * jax.random.uniform(key_of[2], (POINTS, POINTS, POINTS, NELEM), jnp.float32) ** level_of(key_of[2], (POINTS, POINTS, POINTS, NELEM), ((3, 768),), -0.2, 0.2)), 1.0, 4.0)
    element_order = jax.vmap(lambda own: jax.random.permutation(own, ELEM_DEV))(jax.random.split(key_of[3], N_SLAB)).reshape((N_SLAB, ELEM_DEV)).astype(jnp.int32)
    return dict(load_terms=load_terms, geometry=geometry, mass_terms=mass_terms, element_order=element_order)


spectrum_centre = 1.65
spectrum_half = 1.35


def legendre_table(positions, points):
    columns = [positions * 0.0 + 1.0, positions]
    for degree_now in range(2, points):
        columns.append(((2 * degree_now - 1) * positions * columns[-1] - (degree_now - 1) * columns[-2]) / degree_now)
    return np.stack(columns, axis=1)


def gll_derivative(points):
    degree = points - 1
    grid_nodes = -np.cos(np.pi * np.arange(points) / degree)
    for repeat in range(100):
        legendre = legendre_table(grid_nodes, points)
        grid_nodes = grid_nodes - (grid_nodes * legendre[:, degree] - legendre[:, degree - 1]) / (points * legendre[:, degree])
    legendre = legendre_table(grid_nodes, points)
    top_values = legendre[:, degree]
    index_list = np.arange(points)
    same_index = index_list[:, None] == index_list[None, :]
    spacing = grid_nodes[:, None] - grid_nodes[None, :]
    spacing = np.where(same_index, 1.0, spacing)
    deriv_table = top_values[:, None] / (top_values[None, :] * spacing)
    deriv_table = np.where(same_index, 0.0, deriv_table)
    deriv_table[0, 0] = -degree * points / 4.0
    deriv_table[degree, degree] = degree * points / 4.0
    return deriv_table


def local_apply(values, geometry, mass_terms, deriv_table):
    highest = lax.Precision.HIGHEST
    grad_one = jnp.einsum("ma,abce->mbce", deriv_table, values, precision=highest)
    result = jnp.einsum("ma,mbce->abce", deriv_table, geometry[0] * grad_one, precision=highest)
    grad_two = jnp.einsum("mb,abce->amce", deriv_table, values, precision=highest)
    result = result + jnp.einsum("mb,amce->abce", deriv_table, geometry[1] * grad_two, precision=highest)
    grad_three = jnp.einsum("mc,abce->abme", deriv_table, values, precision=highest)
    result = result + jnp.einsum("mc,abme->abce", deriv_table, geometry[2] * grad_three, precision=highest)
    return result + mass_terms * values


def local_diagonal(geometry, mass_terms, deriv_table):
    highest = lax.Precision.HIGHEST
    squared = deriv_table * deriv_table
    result = jnp.einsum("ma,mbce->abce", squared, geometry[0], precision=highest)
    result = result + jnp.einsum("mb,amce->abce", squared, geometry[1], precision=highest)
    result = result + jnp.einsum("mc,abme->abce", squared, geometry[2], precision=highest)
    return result + mass_terms


def to_grid(values, element_order):
    points = values.shape[0]
    inverse = jnp.argsort(element_order, axis=1).astype(jnp.int32)
    row_base = jnp.arange(N_SLAB, dtype=jnp.int32)[:, None] * ELEM_DEV
    picks = (row_base + inverse).reshape(-1).astype(jnp.int32)
    grid = jnp.take(values, picks, axis=3)
    return grid.reshape(points, points, points, N_SLAB * EL_X, EL_Y, EL_Z)


def to_store(grid, element_order):
    points = grid.shape[0]
    row_base = jnp.arange(N_SLAB, dtype=jnp.int32)[:, None] * ELEM_DEV
    picks = (row_base + element_order.astype(jnp.int32)).reshape(-1).astype(jnp.int32)
    return jnp.take(grid.reshape(points, points, points, NELEM), picks, axis=3)


def assemble_grid(grid):
    low_face = grid[0]
    high_face = grid[-1]
    shared = high_face + jnp.roll(low_face, -1, axis=2)
    grid = jnp.concatenate([jnp.roll(shared, 1, axis=2)[None], grid[1:-1], shared[None]], axis=0)
    low_face = grid[:, 0]
    high_face = grid[:, -1]
    zero_column = jnp.zeros_like(low_face[:, :, :, :1])
    new_high = high_face + jnp.concatenate([low_face[:, :, :, 1:], zero_column], axis=3)
    new_low = low_face + jnp.concatenate([zero_column, high_face[:, :, :, :-1]], axis=3)
    grid = jnp.concatenate([new_low[:, None], grid[:, 1:-1], new_high[:, None]], axis=1)
    low_face = grid[:, :, 0]
    high_face = grid[:, :, -1]
    shared = high_face + jnp.roll(low_face, -1, axis=4)
    grid = jnp.concatenate([jnp.roll(shared, 1, axis=4)[:, :, None], grid[:, :, 1:-1], shared[:, :, None]], axis=2)
    return grid


def grid_weights(points):
    node_ids = jnp.arange(points)
    end_node = (node_ids == 0) | (node_ids == points - 1)
    edge_mult = jnp.where(end_node, 2.0, 1.0).astype(jnp.float32)
    cross_ids = jnp.arange(EL_Y)
    low_shared = (node_ids == 0)[:, None] & (cross_ids > 0)[None, :]
    high_shared = (node_ids == points - 1)[:, None] & (cross_ids < EL_Y - 1)[None, :]
    mid_mult = jnp.where(low_shared | high_shared, 2.0, 1.0).astype(jnp.float32)
    total = edge_mult[:, None, None, None, None, None] * mid_mult[None, :, None, None, :, None] * edge_mult[None, None, :, None, None, None]
    full = jnp.broadcast_to(total, (points, points, points, N_SLAB * EL_X, EL_Y, EL_Z))
    return 1.0 / full


def reference(load_terms, geometry, mass_terms, element_order):
    points = load_terms.shape[0]
    deriv_table = jnp.asarray(gll_derivative(points), jnp.float32)

    def stiffness_sum(values):
        return to_store(assemble_grid(to_grid(values, element_order)), element_order)

    def operate(values):
        return stiffness_sum(local_apply(values, geometry, mass_terms, deriv_table))

    weight = to_store(grid_weights(points), element_order)
    start = stiffness_sum(load_terms)
    inv_diag = 1.0 / stiffness_sum(local_diagonal(geometry, mass_terms, deriv_table))
    ratio_sigma = spectrum_centre / spectrum_half
    step_vec = inv_diag * start / spectrum_centre
    precond = step_vec
    rho_prev = 1.0 / ratio_sigma
    for section in range(SECTIONS - 1):
        rho_next = 1.0 / (2.0 * ratio_sigma - rho_prev)
        misfit = start - operate(precond)
        step_vec = rho_next * rho_prev * step_vec + (2.0 * rho_next / spectrum_half) * inv_diag * misfit
        precond = precond + step_vec
        rho_prev = rho_next
    numerator = jnp.sum(weight * start * precond)
    image_vec = operate(precond)
    denominator = jnp.sum(weight * precond * image_vec)
    step_size = numerator / denominator
    return step_size * precond, start - step_size * image_vec
```

```python
import functools

import jax
import jax.numpy as jnp
import numpy as np
from jax import lax
from jax.experimental import pallas as pl
from jax.experimental.pallas import tpu as pltpu
from jax.sharding import Mesh
from jax.sharding import PartitionSpec as P

TORUS = (8, 12, 4, 2)
AXES = ("ty", "tz", "tx", "core")
NODES = 8
EL_Y = 8
EL_Z = 16
CELLS = EL_Y * EL_Z
CENTRE = 1.65
HALF = 1.35
F32 = jnp.float32


def legendre_table(positions, points):
    columns = [positions * 0.0 + 1.0, positions]
    for degree_now in range(2, points):
        columns.append(
            ((2 * degree_now - 1) * positions * columns[-1] - (degree_now - 1) * columns[-2])
            / degree_now
        )
    return np.stack(columns, axis=1)


def gll_derivative(points):
    degree = points - 1
    grid_nodes = -np.cos(np.pi * np.arange(points) / degree)
    for repeat in range(100):
        legendre = legendre_table(grid_nodes, points)
        grid_nodes = grid_nodes - (grid_nodes * legendre[:, degree] - legendre[:, degree - 1]) / (
            points * legendre[:, degree]
        )
    legendre = legendre_table(grid_nodes, points)
    top_values = legendre[:, degree]
    index_list = np.arange(points)
    same_index = index_list[:, None] == index_list[None, :]
    spacing = grid_nodes[:, None] - grid_nodes[None, :]
    spacing = np.where(same_index, 1.0, spacing)
    deriv_table = top_values[:, None] / (top_values[None, :] * spacing)
    deriv_table = np.where(same_index, 0.0, deriv_table)
    deriv_table[0, 0] = -degree * points / 4.0
    deriv_table[degree, degree] = degree * points / 4.0
    return deriv_table


DERIV = gll_derivative(NODES)
HALF_N = NODES // 2
MIRROR = DERIV[:, ::-1]
ON_SUM = 0.5 * (DERIV + MIRROR)[:HALF_N, :HALF_N]
ON_DIFF = 0.5 * (DERIV - MIRROR)[:HALF_N, :HALF_N]
SQUARED = DERIV * DERIV
SQ_SUM = 0.5 * (SQUARED + SQUARED[::-1])[:HALF_N, :HALF_N]
SQ_DIFF = 0.5 * (SQUARED - SQUARED[::-1])[:HALF_N, :HALF_N]

SIGMA = CENTRE / HALF
RHO_0 = 1.0 / SIGMA
RHO_1 = 1.0 / (2.0 * SIGMA - RHO_0)
KEEP = 1.0 + RHO_1 * RHO_0 + 2.0 * RHO_1 / HALF * CENTRE
PULL = -2.0 * RHO_1 / HALF


def combine(weights, values):
    total = None
    for weight, value in zip(weights, values):
        if weight == 0.0:
            continue
        term = value if weight == 1.0 else value * F32(weight)
        total = term if total is None else total + term
    return total


def fold(values):
    low, high = values[:HALF_N], values[: HALF_N - 1 : -1]
    return [a + b for a, b in zip(low, high)], [a - b for a, b in zip(low, high)]


def derive(values):
    even, odd = fold(values)
    by_even = [combine(ON_SUM[m], even) for m in range(HALF_N)]
    by_odd = [combine(ON_DIFF[m], odd) for m in range(HALF_N)]
    return [a + b for a, b in zip(by_even, by_odd)] + [
        b - a for a, b in zip(by_even[::-1], by_odd[::-1])
    ]


def derive_back(values):
    even, odd = fold(values)
    by_even = [combine(ON_DIFF[:, a], even) for a in range(HALF_N)]
    by_odd = [combine(ON_SUM[:, a], odd) for a in range(HALF_N)]
    return [a + b for a, b in zip(by_even, by_odd)] + [
        b - a for a, b in zip(by_even[::-1], by_odd[::-1])
    ]


def square_back(values):
    even, odd = fold(values)
    by_even = [combine(SQ_SUM[:, a], even) for a in range(HALF_N)]
    by_odd = [combine(SQ_DIFF[:, a], odd) for a in range(HALF_N)]
    return [a + b for a, b in zip(by_even, by_odd)] + [
        a - b for a, b in zip(by_even[::-1], by_odd[::-1])
    ]


def stiff_line(values, factors):
    return derive_back([g * d for g, d in zip(factors, derive(values))])


def lanes_of(value, index):
    return jnp.take_along_axis(value, index, axis=1, mode="promise_in_bounds")


class Shared:
    def __init__(self):
        lane = lax.broadcasted_iota(jnp.int32, (8, 128), 1)
        row = lax.broadcasted_iota(jnp.int32, (8, 128), 0)
        pos_z = lane % EL_Z
        up = lane - pos_z + (pos_z + 1) % EL_Z
        down = lane - pos_z + (pos_z + EL_Z - 1) % EL_Z
        self.across = jnp.where(row == 0, up, down)
        self.has_low = lane >= EL_Z
        self.has_high = lane < CELLS - EL_Z
        self.first = row == 0
        self.last = row == NODES - 1

    def plane(self, rows):
        low, high = rows[0], rows[-1]
        zero = jnp.zeros_like(low)
        new_low = low + jnp.where(self.has_low, pltpu.roll(high, EL_Z, 1), zero)
        new_high = high + jnp.where(self.has_high, pltpu.roll(low, CELLS - EL_Z, 1), zero)
        out = []
        for value in [new_low, *rows[1:-1], new_high]:
            moved = lanes_of(value, self.across)
            from_last = pltpu.roll(moved, 1, 0)
            from_first = pltpu.roll(moved, NODES - 1, 0)
            added = jnp.where(self.first, from_last, jnp.where(self.last, from_first, zero))
            out.append(value + added)
        return out


def rows_of(ref, *at):
    return [ref[(*at, pl.ds(8 * b, 8), slice(None))] for b in range(NODES)]


def put_rows(ref, values, *at):
    for b, value in enumerate(values):
        ref[(*at, pl.ds(8 * b, 8), slice(None))] = value


def turned(ref, *at):
    return [ref[(*at, pl.ds(c, 8, stride=8), slice(None))] for c in range(NODES)]


def prepare(core_ref, order_ref, load_in, geom_in, mass_in, load, geo_a, geo_b, geo_c, mass, diag, lead, message, raw, sems):
    sources = [geom_in.at[0], geom_in.at[1], geom_in.at[2], mass_in, load_in]
    copies = [pltpu.make_async_copy(src, raw.at[i], sems.at[i]) for i, src in enumerate(sources)]
    for copy in copies:
        copy.start()
    core = core_ref[0]
    cells = jnp.broadcast_to(order_ref[...], (CELLS, CELLS))
    hot = (cells == lax.broadcasted_iota(jnp.int32, (CELLS, CELLS), 0)).astype(F32)
    column = lax.broadcasted_iota(jnp.int32, (8, CELLS), 1).astype(F32)
    index = lax.dot_general(column, hot, (((1,), (1,)), ((), ())), preferred_element_type=F32)
    index = index.astype(jnp.int32)
    at = [a + core * (NODES - 1 - 2 * a) for a in range(NODES)]

    def fetch(which, a):
        return [lanes_of(v, index) for v in rows_of(raw, which, at[a])]

    copies[0].wait()
    for a in range(NODES):
        put_rows(geo_a, fetch(0, a), a)
    copies[1].wait()
    for a in range(NODES):
        put_rows(geo_b, fetch(1, a), a)
    copies[2].wait()
    for a in range(NODES):
        for c in range(NODES):
            geo_c[a, pl.ds(8 * c, 8), :] = lanes_of(raw[2, at[a], pl.ds(c, 8, stride=8), :], index)
    copies[3].wait()
    for a in range(NODES):
        put_rows(mass, fetch(3, a), a)
    copies[4].wait()
    for a in range(NODES):
        put_rows(load, fetch(4, a), a)
    for a in range(1, NODES):
        put_rows(diag, square_back(rows_of(geo_c, a)), a)
    for a in range(1, NODES):
        part = square_back(rows_of(geo_b, a))
        turn = turned(diag, a)
        put_rows(diag, [x + y + z for x, y, z in zip(part, turn, rows_of(mass, a))], a)
    for b in range(NODES):
        here = pl.ds(8 * b, 8)
        part = square_back([geo_a[a, here, :] for a in range(NODES)])
        lead[here, :] = part[0] + mass[0, here, :]
        for a in range(1, NODES):
            diag[a, here, :] = diag[a, here, :] + part[a]
    put_rows(message, rows_of(load, NODES - 1), 0)
    put_rows(message, rows_of(diag, NODES - 1), 1)


def begin(load, geo_a, geo_b, geo_c, diag, lead, pair, start, recip, first, slope, message):
    shared = Shared()
    for a in range(1, NODES):
        if a < NODES - 1:
            top, low = rows_of(load, a), rows_of(diag, a)
        else:
            top = [x + y for x, y in zip(rows_of(pair, 0, 0), rows_of(pair, 1, 0))]
            low = [x + y for x, y in zip(rows_of(pair, 0, 1), rows_of(pair, 1, 1))]
        top, low = shared.plane(top), [1.0 / v for v in shared.plane(low)]
        put_rows(start, top, a)
        put_rows(recip, low, a)
        put_rows(first, [x * y * F32(1.0 / CENTRE) for x, y in zip(top, low)], a)
    for b in range(NODES):
        here = pl.ds(8 * b, 8)
        zero = jnp.zeros((8, 128), F32)
        grad = derive([zero] + [first[a, here, :] for a in range(1, NODES)])
        for a in range(NODES):
            slope[a, here, :] = grad[a]
        flux = [geo_a[a, here, :] * grad[a] for a in range(NODES)]
        message[1, here, :] = combine(DERIV[:, 0], flux)
    put_rows(message, rows_of(load, 0), 0)
    put_rows(message, [lead[pl.ds(8 * b, 8), :] for b in range(NODES)], 2)
    put_rows(message, rows_of(geo_b, 0), 3)
    put_rows(message, rows_of(geo_c, 0), 4)


def middle(both, geo_a, geo_b, geo_c, mass, recip_in, first_in, slope, start0, recip0, first0, local, precond, message, work):
    shared = Shared()

    def summed(which):
        return [x + y for x, y in zip(rows_of(both, 0, which), rows_of(both, 1, which))]

    lead, fac_b, fac_c = summed(2), summed(3), summed(4)
    put_rows(work, square_back(fac_c), 0)
    low = [x + y + z for x, y, z in zip(square_back(fac_b), turned(work, 0), lead)]
    low = [1.0 / v for v in shared.plane(low)]
    top = shared.plane(summed(0))
    head = [x * y * F32(1.0 / CENTRE) for x, y in zip(top, low)]
    put_rows(start0, top)
    put_rows(recip0, low)
    put_rows(first0, head)
    put_rows(work, stiff_line(turned(first0), fac_c), 0)
    turn = turned(work, 0)
    part = stiff_line(head, fac_b)
    image = [r + k * u + x + y for r, k, u, x, y in zip(summed(1), lead, head, part, turn)]
    image = shared.plane(image)
    put_rows(precond, [u * F32(KEEP) + q * d * F32(PULL) for u, q, d in zip(head, image, low)], 0)

    for b in range(NODES):
        here = pl.ds(8 * b, 8)
        flux = []
        for a in range(NODES):
            flux.append(geo_a[a, here, :] * (slope[a, here, :] + head[b] * F32(DERIV[a, 0])))
        back = derive_back(flux)
        for a in range(1, NODES):
            local[a, here, :] = back[a]
    for a in range(1, NODES):
        put_rows(work, stiff_line(turned(first_in, a), rows_of(geo_c, a)), a)
    for a in range(1, NODES):
        values = rows_of(first_in, a)
        part = stiff_line(values, rows_of(geo_b, a))
        turn = turned(work, a)
        image = [
            x + y + z + m * v
            for x, y, z, m, v in zip(rows_of(local, a), part, turn, rows_of(mass, a), values)
        ]
        if a == NODES - 1:
            put_rows(message, image)
        else:
            image = shared.plane(image)
            low = rows_of(recip_in, a)
            put_rows(
                precond,
                [u * F32(KEEP) + q * d * F32(PULL) for u, q, d in zip(values, image, low)],
                a,
            )


def finish(pair, geo_a, geo_b, geo_c, mass, load, recip_in, first_in, precond_in, last, image, outer, inner, row, local, work):
    shared = Shared()
    whole = shared.plane([x + y for x, y in zip(rows_of(pair, 0), rows_of(pair, 1))])
    end = [
        u * F32(KEEP) + q * d * F32(PULL)
        for u, q, d in zip(rows_of(first_in, NODES - 1), whole, rows_of(recip_in, NODES - 1))
    ]
    put_rows(last, end)

    def iterate(a):
        return rows_of(last) if a == NODES - 1 else rows_of(precond_in, a)

    for b in range(NODES):
        here = pl.ds(8 * b, 8)
        values = [precond_in[a, here, :] for a in range(NODES - 1)] + [end[b]]
        back = stiff_line(values, [geo_a[a, here, :] for a in range(NODES)])
        for a in range(NODES):
            local[a, here, :] = back[a]
    for a in range(NODES):
        lines = turned(last) if a == NODES - 1 else turned(precond_in, a)
        put_rows(work, stiff_line(lines, rows_of(geo_c, a)), a)
    over = [jnp.zeros((8, 128), F32) for _ in range(NODES)]
    under = [jnp.zeros((8, 128), F32) for _ in range(NODES)]
    for a in range(NODES):
        values = iterate(a)
        part = stiff_line(values, rows_of(geo_b, a))
        turn = turned(work, a)
        total = [
            x + y + z + m * v
            for x, y, z, m, v in zip(rows_of(local, a), part, turn, rows_of(mass, a), values)
        ]
        over = [s + v * f for s, v, f in zip(over, values, rows_of(load, a))]
        under = [s + v * t for s, v, t in zip(under, values, total)]
        if a == 0:
            put_rows(outer, total)
        elif a == NODES - 1:
            put_rows(inner, total)
        else:
            put_rows(image, shared.plane(total), a)
    over = jnp.sum(functools.reduce(jnp.add, over), axis=0, keepdims=True)
    under = jnp.sum(functools.reduce(jnp.add, under), axis=0, keepdims=True)
    over = over + pltpu.roll(over, 64, 1)
    under = under + pltpu.roll(under, 64, 1)
    lane = lax.broadcasted_iota(jnp.int32, (1, 128), 1)
    row[...] = jnp.broadcast_to(jnp.where(lane < 64, over, under), row.shape)


def close(core_ref, order_ref, sums, outer, outer_other, pair, start_in, start0, precond_in, last, image_in, solution_out, residual_out, buf_s, buf_r, sems):
    shared = Shared()
    core = core_ref[0]
    index = jnp.broadcast_to(order_ref[...], (8, CELLS))
    lane = lax.broadcasted_iota(jnp.int32, (1, 128), 1)
    total = jnp.sum(sums[...], axis=0, keepdims=True)
    zero = jnp.zeros_like(total)
    over = jnp.sum(jnp.where(lane < 64, total, zero), axis=1, keepdims=True)
    under = jnp.sum(jnp.where(lane < 64, zero, total), axis=1, keepdims=True)
    alpha = jnp.broadcast_to(over / under, (8, 128))
    at = [a + core * (NODES - 1 - 2 * a) for a in range(NODES)]
    copies = []
    for a in range(NODES):
        if a == 0:
            head, values = rows_of(start0), rows_of(precond_in, 0)
            image = shared.plane([x + y for x, y in zip(rows_of(outer), rows_of(outer_other))])
        elif a == NODES - 1:
            head, values = rows_of(start_in, a), rows_of(last)
            image = shared.plane([x + y for x, y in zip(rows_of(pair, 0), rows_of(pair, 1))])
        else:
            head, values, image = rows_of(start_in, a), rows_of(precond_in, a), rows_of(image_in, a)
        put_rows(buf_s, [lanes_of(alpha * v, index) for v in values], a)
        put_rows(buf_r, [lanes_of(s - alpha * i, index) for s, i in zip(head, image)], a)
        for i, (buf, out) in enumerate(((buf_s, solution_out), (buf_r, residual_out))):
            copy = pltpu.make_async_copy(buf.at[a], out.at[at[a]], sems.at[i, a])
            copy.start()
            copies.append(copy)
    for copy in copies:
        copy.wait()


VMEM = pl.BlockSpec(memory_space=pltpu.VMEM)
SMEM = pl.BlockSpec(memory_space=pltpu.SMEM)
ANY = pl.BlockSpec(memory_space=pl.ANY)
FIELD = (NODES, 64, 128)
FACE = (64, 128)


def call(body, name, outs, ins, scratch=(), out_specs=None, flops=4_000_000):
    return pl.pallas_call(
        body,
        name=name,
        out_shape=[jax.ShapeDtypeStruct(s, F32) for s in outs],
        in_specs=ins,
        out_specs=out_specs or [VMEM] * len(outs),
        scratch_shapes=list(scratch),
        compiler_params=pltpu.CompilerParams(vmem_limit_bytes=12 << 20),
        cost_estimate=pl.CostEstimate(flops=flops, bytes_accessed=2 << 20, transcendentals=0),
    )


def on_device(load_terms, geometry, mass_terms, element_order):
    count = 1
    for axis in AXES:
        count *= lax.axis_size(axis)
    across_chips = [[2 * k + 1, (2 * k + 2) % count] for k in range(count // 2)]
    swap = [(i, (i + 1) % count if i % 2 else (i - 1) % count) for i in range(count)]
    core = lax.axis_index("core").astype(jnp.int32).reshape(1)
    field = jax.ShapeDtypeStruct(FIELD, F32)
    dma = pltpu.SemaphoreType.DMA
    load_terms = load_terms.reshape(FIELD)
    geometry = geometry.reshape(3, *FIELD)
    mass_terms = mass_terms.reshape(FIELD)

    load, geo_a, geo_b, geo_c, mass, diag, lead, message = call(
        prepare,
        "prepare",
        [FIELD] * 6 + [FACE, (2, *FACE)],
        [SMEM, VMEM, ANY, ANY, ANY],
        [pltpu.VMEM((5, *FIELD), F32), dma((5,))],
    )(core, element_order, load_terms, geometry, mass_terms)
    pair = lax.all_gather(message, "core")
    start, recip, first, slope, message = call(
        begin, "begin", [FIELD] * 4 + [(5, *FACE)], [VMEM] * 7
    )(load, geo_a, geo_b, geo_c, diag, lead, pair)
    both = lax.all_gather(message, AXES, axis_index_groups=across_chips)
    start0, recip0, first0, local, precond, message = call(
        middle,
        "middle",
        [FACE] * 3 + [FIELD, FIELD, FACE],
        [VMEM] * 8,
        [pltpu.VMEM(FIELD, F32)],
    )(both, geo_a, geo_b, geo_c, mass, recip, first, slope)
    pair = lax.all_gather(message, "core")
    group = lax.axis_size("ty") * lax.axis_size("tx")
    last, image, outer, inner, row = call(
        finish,
        "finish",
        [FACE, FIELD, FACE, FACE, (group, 128)],
        [VMEM] * 9,
        [pltpu.VMEM(FIELD, F32), pltpu.VMEM(FIELD, F32)],
    )(pair, geo_a, geo_b, geo_c, mass, load, recip, first, precond)
    outer_other = lax.ppermute(outer, AXES, swap)
    pair = lax.all_gather(inner, "core")
    sums = lax.all_to_all(row, ("ty", "tx"), 0, 0, tiled=True)
    group = lax.axis_size("tz") * lax.axis_size("core")
    row = jnp.broadcast_to(jnp.sum(sums, axis=0, keepdims=True), (group, 128))
    sums = lax.all_to_all(row, ("tz", "core"), 0, 0, tiled=True)
    solution, residual = call(
        close,
        "close",
        [FIELD, FIELD],
        [SMEM] + [VMEM] * 10,
        [pltpu.VMEM(FIELD, F32), pltpu.VMEM(FIELD, F32), dma((2, NODES))],
        out_specs=[ANY, ANY],
    )(core, element_order, sums, outer, outer_other, pair, start, start0, precond, last, image)
    shape = (NODES, NODES, NODES, CELLS)
    return solution.reshape(shape), residual.reshape(shape)


def solution(mesh):
    torus = Mesh(mesh.devices.reshape(TORUS), AXES)
    placed = (
        P(None, None, None, AXES),
        P(None, None, None, None, AXES),
        P(None, None, None, AXES),
        P(AXES, None),
    )
    return jax.shard_map(
        on_device,
        mesh=torus,
        in_specs=placed,
        out_specs=(P(None, None, None, AXES), P(None, None, None, AXES)),
        check_vma=False,
    )
```

```python
import functools

import jax
import jax.numpy as jnp
import numpy as np
from jax import lax
from jax.experimental import pallas as pl
from jax.experimental.pallas import tpu as pltpu
from jax.sharding import Mesh
from jax.sharding import PartitionSpec as P


TORUS = (8, 12, 4, 2)
AXES = ("ty", "tz", "tx", "core")
ROOT = (6, 10, 2, 1)


def groups(axes):
    ids = np.arange(np.prod(TORUS)).reshape(TORUS)
    ids = np.roll(ids, [-r for r in ROOT], range(4))
    others = [d for d in range(4) if d not in axes]
    return ids.transpose(*others, *axes).reshape(-1, np.prod([TORUS[d] for d in axes])).tolist()


NODES = 8
EL_Y = 8
EL_Z = 16
CELLS = EL_Y * EL_Z
CENTRE = 1.65
HALF = 1.35
F32 = jnp.float32


def legendre_table(positions, points):
    columns = [positions * 0.0 + 1.0, positions]
    for degree_now in range(2, points):
        columns.append(
            ((2 * degree_now - 1) * positions * columns[-1] - (degree_now - 1) * columns[-2])
            / degree_now
        )
    return np.stack(columns, axis=1)


def gll_derivative(points):
    degree = points - 1
    grid_nodes = -np.cos(np.pi * np.arange(points) / degree)
    for _ in range(100):
        legendre = legendre_table(grid_nodes, points)
        grid_nodes = grid_nodes - (grid_nodes * legendre[:, degree] - legendre[:, degree - 1]) / (
            points * legendre[:, degree]
        )
    legendre = legendre_table(grid_nodes, points)
    top_values = legendre[:, degree]
    index_list = np.arange(points)
    same_index = index_list[:, None] == index_list[None, :]
    spacing = grid_nodes[:, None] - grid_nodes[None, :]
    spacing = np.where(same_index, 1.0, spacing)
    deriv_table = top_values[:, None] / (top_values[None, :] * spacing)
    deriv_table = np.where(same_index, 0.0, deriv_table)
    deriv_table[0, 0] = -degree * points / 4.0
    deriv_table[degree, degree] = degree * points / 4.0
    return deriv_table


DERIV = gll_derivative(NODES)
HALF_N = NODES // 2
MIRROR = DERIV[:, ::-1]
ON_SUM = 0.5 * (DERIV + MIRROR)[:HALF_N, :HALF_N]
ON_DIFF = 0.5 * (DERIV - MIRROR)[:HALF_N, :HALF_N]
SQUARED = DERIV * DERIV
SQ_SUM = 0.5 * (SQUARED + SQUARED[::-1])[:HALF_N, :HALF_N]
SQ_DIFF = 0.5 * (SQUARED - SQUARED[::-1])[:HALF_N, :HALF_N]

SIGMA = CENTRE / HALF
RHO_0 = 1.0 / SIGMA
RHO_1 = 1.0 / (2.0 * SIGMA - RHO_0)
KEEP = 1.0 + RHO_1 * RHO_0 + 2.0 * RHO_1 / HALF * CENTRE
PULL = -2.0 * RHO_1 / HALF


def combine(weights, values):
    total = None
    for weight, value in zip(weights, values):
        if weight == 0.0:
            continue
        term = value if weight == 1.0 else value * F32(weight)
        total = term if total is None else total + term
    return total


def fold(values):
    low, high = values[:HALF_N], values[: HALF_N - 1 : -1]
    return [a + b for a, b in zip(low, high)], [a - b for a, b in zip(low, high)]


def derive(values):
    even, odd = fold(values)
    by_even = [combine(ON_SUM[m], even) for m in range(HALF_N)]
    by_odd = [combine(ON_DIFF[m], odd) for m in range(HALF_N)]
    return [a + b for a, b in zip(by_even, by_odd)] + [
        b - a for a, b in zip(by_even[::-1], by_odd[::-1])
    ]


def derive_back(values):
    even, odd = fold(values)
    by_even = [combine(ON_DIFF[:, a], even) for a in range(HALF_N)]
    by_odd = [combine(ON_SUM[:, a], odd) for a in range(HALF_N)]
    return [a + b for a, b in zip(by_even, by_odd)] + [
        b - a for a, b in zip(by_even[::-1], by_odd[::-1])
    ]


def square_back(values):
    even, odd = fold(values)
    by_even = [combine(SQ_SUM[:, a], even) for a in range(HALF_N)]
    by_odd = [combine(SQ_DIFF[:, a], odd) for a in range(HALF_N)]
    return [a + b for a, b in zip(by_even, by_odd)] + [
        a - b for a, b in zip(by_even[::-1], by_odd[::-1])
    ]


def stiff_line(values, factors):
    return derive_back([g * d for g, d in zip(factors, derive(values))])


def lanes_of(value, index):
    return jnp.take_along_axis(value, index, axis=1, mode="promise_in_bounds")


class Shared:
    def __init__(self):
        lane = lax.broadcasted_iota(jnp.int32, (8, 128), 1)
        row = lax.broadcasted_iota(jnp.int32, (8, 128), 0)
        pos_z = lane % EL_Z
        up = lane - pos_z + (pos_z + 1) % EL_Z
        down = lane - pos_z + (pos_z + EL_Z - 1) % EL_Z
        self.across = jnp.where(row == 0, up, down)
        self.has_low = lane >= EL_Z
        self.has_high = lane < CELLS - EL_Z
        self.first = row == 0
        self.last = row == NODES - 1

    def plane(self, rows):
        low, high = rows[0], rows[-1]
        zero = jnp.zeros_like(low)
        new_low = low + jnp.where(self.has_low, pltpu.roll(high, EL_Z, 1), zero)
        new_high = high + jnp.where(self.has_high, pltpu.roll(low, CELLS - EL_Z, 1), zero)
        out = []
        for value in [new_low, *rows[1:-1], new_high]:
            moved = lanes_of(value, self.across)
            from_last = pltpu.roll(moved, 1, 0)
            from_first = pltpu.roll(moved, NODES - 1, 0)
            added = jnp.where(self.first, from_last, jnp.where(self.last, from_first, zero))
            out.append(value + added)
        return out


def rows_of(ref, *at):
    return [ref[(*at, pl.ds(8 * b, 8), slice(None))] for b in range(NODES)]


def put_rows(ref, values, *at):
    for b, value in enumerate(values):
        ref[(*at, pl.ds(8 * b, 8), slice(None))] = value


def turned(ref, *at):
    return [ref[(*at, pl.ds(c, 8, stride=8), slice(None))] for c in range(NODES)]


def prepare(order_in, load_in, geom_in, mass_in, load, geo_a, geo_b, geo_c, mass, diag, lead, message, order_ref, raw, sems):
    order_copy = pltpu.make_async_copy(order_in, order_ref, sems.at[5])
    order_copy.start()
    sources = [geom_in.at[0], geom_in.at[1], geom_in.at[2], mass_in, load_in]
    copies = [pltpu.make_async_copy(src, raw.at[i], sems.at[i]) for i, src in enumerate(sources)]
    for copy in copies:
        copy.start()
    core = lax.axis_index("core")
    order_copy.wait()
    cells = jnp.broadcast_to(order_ref[...], (CELLS, CELLS))
    hot = (cells == lax.broadcasted_iota(jnp.int32, (CELLS, CELLS), 0)).astype(F32)
    column = lax.broadcasted_iota(jnp.int32, (8, CELLS), 1).astype(F32)
    index = lax.dot_general(column, hot, (((1,), (1,)), ((), ())), preferred_element_type=F32)
    index = index.astype(jnp.int32)
    at = [a + core * (NODES - 1 - 2 * a) for a in range(NODES)]

    def fetch(which, a):
        return [lanes_of(v, index) for v in rows_of(raw, which, at[a])]

    copies[0].wait()
    for a in range(NODES):
        put_rows(geo_a, fetch(0, a), a)
    copies[1].wait()
    for a in range(NODES):
        put_rows(geo_b, fetch(1, a), a)
    copies[2].wait()
    for a in range(NODES):
        for c in range(NODES):
            geo_c[a, pl.ds(8 * c, 8), :] = lanes_of(raw[2, at[a], pl.ds(c, 8, stride=8), :], index)
    copies[3].wait()
    for a in range(NODES):
        put_rows(mass, fetch(3, a), a)
    copies[4].wait()
    for a in range(NODES):
        put_rows(load, fetch(4, a), a)
    for a in range(1, NODES - 1):
        put_rows(diag, square_back(rows_of(geo_c, a)), a)
    for a in range(1, NODES - 1):
        part = square_back(rows_of(geo_b, a))
        turn = turned(diag, a)
        put_rows(diag, [x + y + z for x, y, z in zip(part, turn, rows_of(mass, a))], a)
    for b in range(NODES):
        here = pl.ds(8 * b, 8)
        part = square_back([geo_a[a, here, :] for a in range(NODES)])
        lead[here, :] = part[0] + mass[0, here, :]
        for a in range(1, NODES - 1):
            diag[a, here, :] = diag[a, here, :] + part[a]
        message[1, here, :] = part[NODES - 1]
    for i, ref in ((0, load), (2, mass), (3, geo_b), (4, geo_c)):
        put_rows(message, rows_of(ref, NODES - 1), i)


def summed(ref, which):
    return [x + y for x, y in zip(rows_of(ref, 0, which), rows_of(ref, 1, which))]


def settle(shared, load, lead, fac_b, fac_c, work):
    put_rows(work, square_back(fac_c))
    low = [x + y + z for x, y, z in zip(square_back(fac_b), turned(work), lead)]
    low = [1.0 / v for v in shared.plane(low)]
    top = shared.plane(load)
    return top, low, [x * y * F32(1.0 / CENTRE) for x, y in zip(top, low)]


def within(values, lead, fac_b, fac_c, keep, work):
    put_rows(keep, values)
    put_rows(work, stiff_line(turned(keep), fac_c))
    part = stiff_line(values, fac_b)
    return [k * u + x + y for k, u, x, y in zip(lead, values, part, turned(work))]


def begin(load, geo_a, geo_b, geo_c, diag, lead, pair, start, recip, first, slope, message, end, keep, work):
    shared = Shared()
    mass_7, fac_b, fac_c = summed(pair, 2), summed(pair, 3), summed(pair, 4)
    lead_7 = [x + y for x, y in zip(summed(pair, 1), mass_7)]
    top, low, tail = settle(shared, summed(pair, 0), lead_7, fac_b, fac_c, work)
    put_rows(start, top, NODES - 1)
    put_rows(recip, low, NODES - 1)
    put_rows(first, tail, NODES - 1)
    put_rows(end, lead_7, 0)
    put_rows(end, fac_b, 1)
    put_rows(end, fac_c, 2)
    put_rows(end, within(tail, mass_7, fac_b, fac_c, keep, work), 3)
    for a in range(1, NODES - 1):
        top, low = shared.plane(rows_of(load, a)), shared.plane(rows_of(diag, a))
        low = [1.0 / v for v in low]
        put_rows(start, top, a)
        put_rows(recip, low, a)
        put_rows(first, [x * y * F32(1.0 / CENTRE) for x, y in zip(top, low)], a)
    for b in range(NODES):
        here = pl.ds(8 * b, 8)
        zero = jnp.zeros((8, 128), F32)
        grad = derive([zero] + [first[a, here, :] for a in range(1, NODES)])
        for a in range(NODES):
            slope[a, here, :] = grad[a]
        flux = [geo_a[a, here, :] * grad[a] for a in range(NODES)]
        message[1, here, :] = combine(DERIV[:, 0], flux)
    put_rows(message, rows_of(load, 0), 0)
    put_rows(message, rows_of(lead), 2)
    put_rows(message, rows_of(geo_b, 0), 3)
    put_rows(message, rows_of(geo_c, 0), 4)


def improve(first, image, recip):
    return [u * F32(KEEP) + q * d * F32(PULL) for u, q, d in zip(first, image, recip)]


def middle(both, geo_a, geo_b, geo_c, mass, recip, first, slope, start0, precond, ahead, message, keep, local, work):
    shared = Shared()
    lead, fac_b, fac_c = summed(both, 2), summed(both, 3), summed(both, 4)
    top, low, head = settle(shared, summed(both, 0), lead, fac_b, fac_c, work.at[0])
    put_rows(start0, top)
    image = within(head, lead, fac_b, fac_c, keep, work.at[0])
    image = shared.plane([x + y for x, y in zip(summed(both, 1), image)])
    put_rows(precond, improve(head, image, low), 0)
    for b in range(NODES):
        here = pl.ds(8 * b, 8)
        flux = []
        for a in range(NODES):
            flux.append(geo_a[a, here, :] * (slope[a, here, :] + head[b] * F32(DERIV[a, 0])))
        back = derive_back(flux)
        for a in range(1, NODES - 1):
            local[a, here, :] = back[a]
        message[0, here, :] = back[NODES - 1]
    for a in range(1, NODES - 1):
        put_rows(work, stiff_line(turned(first, a), rows_of(geo_c, a)), a)
    for a in range(1, NODES - 1):
        values = rows_of(first, a)
        part = stiff_line(values, rows_of(geo_b, a))
        turn = turned(work, a)
        image = [
            x + y + z + m * v
            for x, y, z, m, v in zip(rows_of(local, a), part, turn, rows_of(mass, a), values)
        ]
        put_rows(precond, improve(values, shared.plane(image), rows_of(recip, a)), a)
    for b in range(NODES):
        here = pl.ds(8 * b, 8)
        zero = jnp.zeros((8, 128), F32)
        grad = derive([precond[a, here, :] for a in range(NODES - 1)] + [zero])
        for a in range(NODES):
            ahead[a, here, :] = grad[a]
        flux = [geo_a[a, here, :] * grad[a] for a in range(NODES)]
        message[1, here, :] = combine(DERIV[:, NODES - 1], flux)


def finish(pair, end, geo_a, geo_b, geo_c, mass, load, recip, first, precond_in, ahead, precond, image, outer, row, keep, local, work):
    shared = Shared()
    whole = shared.plane([x + y for x, y in zip(summed(pair, 0), rows_of(end, 3))])
    tail = improve(rows_of(first, NODES - 1), whole, rows_of(recip, NODES - 1))
    put_rows(precond, tail)
    inside = within(tail, rows_of(end, 0), rows_of(end, 1), rows_of(end, 2), keep, work.at[0])
    put_rows(image, shared.plane([x + y for x, y in zip(summed(pair, 1), inside)]), NODES - 1)
    for b in range(NODES):
        here = pl.ds(8 * b, 8)
        flux = []
        for a in range(NODES):
            step = tail[b] * F32(DERIV[a, NODES - 1]) if DERIV[a, NODES - 1] else None
            flux.append(geo_a[a, here, :] * (ahead[a, here, :] + step))
        back = derive_back(flux)
        for a in range(NODES):
            local[a, here, :] = back[a]
    for a in range(NODES):
        lines = turned(precond) if a == NODES - 1 else turned(precond_in, a)
        put_rows(work, stiff_line(lines, rows_of(geo_c, a)), a)
    over = [jnp.zeros((8, 128), F32) for _ in range(NODES)]
    under = [jnp.zeros((8, 128), F32) for _ in range(NODES)]
    for a in range(NODES):
        values = tail if a == NODES - 1 else rows_of(precond_in, a)
        part = stiff_line(values, rows_of(geo_b, a))
        turn = turned(work, a)
        total = [
            x + y + z + m * v
            for x, y, z, m, v in zip(rows_of(local, a), part, turn, rows_of(mass, a), values)
        ]
        over = [s + v * f for s, v, f in zip(over, values, rows_of(load, a))]
        under = [s + v * t for s, v, t in zip(under, values, total)]
        if a == 0:
            put_rows(outer, total)
        elif a < NODES - 1:
            put_rows(image, shared.plane(total), a)
    over = jnp.sum(functools.reduce(jnp.add, over), axis=0, keepdims=True)
    under = jnp.sum(functools.reduce(jnp.add, under), axis=0, keepdims=True)
    over = over + pltpu.roll(over, 64, 1)
    under = under + pltpu.roll(under, 64, 1)
    lane = lax.broadcasted_iota(jnp.int32, (1, 128), 1)
    row[...] = jnp.broadcast_to(jnp.where(lane < 64, over, under), row.shape)


def step_length(sums, alpha):
    lane = lax.broadcasted_iota(jnp.int32, (1, 128), 1)
    total = jnp.sum(sums[...], axis=0, keepdims=True)
    zero = jnp.zeros_like(total)
    over = jnp.sum(jnp.where(lane < 64, total, zero), axis=1, keepdims=True)
    under = jnp.sum(jnp.where(lane < 64, zero, total), axis=1, keepdims=True)
    alpha[...] = jnp.broadcast_to(over / under, (8, 128))


def close(order_ref, alpha_ref, outer, outer_other, start_in, start0, precond_in, last, image_in, solution_out, residual_out, buf_s, buf_r, sems):
    shared = Shared()
    core = lax.axis_index("core")
    index = jnp.broadcast_to(order_ref[...], (8, CELLS))
    alpha = alpha_ref[...]
    at = [a + core * (NODES - 1 - 2 * a) for a in range(NODES)]
    copies = []
    for a in range(NODES):
        if a == 0:
            head, values = rows_of(start0), rows_of(precond_in, 0)
            image = shared.plane([x + y for x, y in zip(rows_of(outer), rows_of(outer_other))])
        elif a == NODES - 1:
            head, values, image = rows_of(start_in, a), rows_of(last), rows_of(image_in, a)
        else:
            head, values, image = rows_of(start_in, a), rows_of(precond_in, a), rows_of(image_in, a)
        for b, (v, s, i) in enumerate(zip(values, head, image)):
            buf_s[a, b] = lanes_of(alpha * v, index)
            buf_r[a, b] = lanes_of(s - alpha * i, index)
        for i, (buf, out) in enumerate(((buf_s, solution_out), (buf_r, residual_out))):
            copy = pltpu.make_async_copy(buf.at[a], out.at[at[a]], sems.at[i, a])
            copy.start()
            copies.append(copy)
    for copy in copies:
        copy.wait()


def gather_up(sums, row):
    row[...] = jnp.broadcast_to(jnp.sum(sums[...], axis=0, keepdims=True), row.shape)


VMEM = pl.BlockSpec(memory_space=pltpu.VMEM)
HBM = pl.BlockSpec(memory_space=pltpu.HBM)
ANY = pl.BlockSpec(memory_space=pl.ANY)
FIELD = (NODES, 64, 128)
FACE = (64, 128)
BLOCK = (NODES, NODES, NODES, CELLS)


def call(body, outs, ins, scratch=(), out_specs=None, flops=4_000_000):
    return pl.pallas_call(
        body,
        out_shape=[jax.ShapeDtypeStruct(s, F32) if isinstance(s, tuple) else s for s in outs],
        in_specs=ins,
        out_specs=out_specs or [VMEM] * len(outs),
        scratch_shapes=list(scratch),
        compiler_params=pltpu.CompilerParams(vmem_limit_bytes=12 << 20),
        cost_estimate=pl.CostEstimate(flops=flops, bytes_accessed=2 << 20, transcendentals=0),
    )


def on_device(load_terms, geometry, mass_terms, element_order):
    count = 1
    for axis in AXES:
        count *= lax.axis_size(axis)
    across_chips = [[2 * k + 1, (2 * k + 2) % count] for k in range(count // 2)]
    plane_groups, line_groups = groups((1, 3)), groups((0, 2))
    in_chip = [[2 * k + 1, 2 * k] for k in range(count // 2)]
    swap = [(i, (i + 1) % count if i % 2 else (i - 1) % count) for i in range(count)]
    dma = pltpu.SemaphoreType.DMA
    arguments = (
        element_order,
        load_terms.reshape(FIELD),
        geometry.reshape(3, *FIELD),
        mass_terms.reshape(FIELD),
    )
    arguments = [pltpu.with_memory_space_constraint(x, pltpu.HBM) for x in arguments]

    load, geo_a, geo_b, geo_c, mass, diag, lead, message, order = call(
        prepare,
        [FIELD] * 6 + [FACE, (5, *FACE), jax.ShapeDtypeStruct((1, CELLS), jnp.int32)],
        [HBM] * 4,
        [pltpu.VMEM((5, *FIELD), F32), dma((6,))],
    )(*arguments)
    pair = lax.all_gather(message, AXES, axis_index_groups=in_chip)
    start, recip, first, slope, message, end = call(
        begin, [FIELD] * 4 + [(5, *FACE), (4, *FACE)], [VMEM] * 7, [pltpu.VMEM(FACE, F32), pltpu.VMEM(FACE, F32)]
    )(load, geo_a, geo_b, geo_c, diag, lead, pair)
    both = lax.all_gather(message, AXES, axis_index_groups=across_chips)
    start0, precond, ahead, message = call(
        middle,
        [FACE, FIELD, FIELD, (2, *FACE)],
        [VMEM] * 8,
        [pltpu.VMEM(FACE, F32), pltpu.VMEM(FIELD, F32), pltpu.VMEM(FIELD, F32)],
    )(both, geo_a, geo_b, geo_c, mass, recip, first, slope)
    pair = lax.all_gather(message, AXES, axis_index_groups=in_chip)
    last, image, outer, row = call(
        finish,
        [FACE, FIELD, FACE, (len(plane_groups[0]), 128)],
        [VMEM] * 11,
        [pltpu.VMEM(FACE, F32), pltpu.VMEM(FIELD, F32), pltpu.VMEM(FIELD, F32)],
    )(pair, end, geo_a, geo_b, geo_c, mass, load, recip, first, precond, ahead)
    outer_other = lax.ppermute(outer, AXES, swap)
    sums = lax.all_to_all(row, AXES, 0, 0, tiled=True, axis_index_groups=plane_groups)
    (row,) = call(gather_up, [(len(line_groups[0]), 128)], [VMEM], flops=100_000)(sums)
    sums = lax.all_to_all(row, AXES, 0, 0, tiled=True, axis_index_groups=line_groups)
    (alpha,) = call(step_length, [(8, 128)], [VMEM], flops=100_000)(sums)
    solution, residual = call(
        close,
        [BLOCK, BLOCK],
        [VMEM] * 9,
        [pltpu.VMEM(BLOCK, F32), pltpu.VMEM(BLOCK, F32), dma((2, NODES))],
        out_specs=[ANY, ANY],
    )(order, alpha, outer, outer_other, start, start0, precond, last, image)
    return solution, residual


def solution(mesh):
    torus = Mesh(mesh.devices.reshape(TORUS), AXES)
    placed = (
        P(None, None, None, AXES),
        P(None, None, None, None, AXES),
        P(None, None, None, AXES),
        P(AXES, None),
    )
    return jax.shard_map(
        on_device,
        mesh=torus,
        in_specs=placed,
        out_specs=(P(None, None, None, AXES), P(None, None, None, AXES)),
        check_vma=False,
    )
```

```python
import functools

import jax
import jax.numpy as jnp
import numpy as np
from jax import lax
from jax.experimental import pallas as pl
from jax.experimental.pallas import tpu as pltpu
from jax.sharding import Mesh
from jax.sharding import PartitionSpec as P


TORUS = (8, 12, 4, 2)
AXES = ("ty", "tz", "tx", "core")
ROOT = (5, 10, 3, 1)


def groups(axes):
    ids = np.arange(np.prod(TORUS)).reshape(TORUS)
    ids = np.roll(ids, [-r for r in ROOT], range(4))
    others = [d for d in range(4) if d not in axes]
    return ids.transpose(*others, *axes).reshape(-1, np.prod([TORUS[d] for d in axes])).tolist()


NODES = 8
EL_Y = 8
EL_Z = 16
CELLS = EL_Y * EL_Z
CENTRE = 1.65
HALF = 1.35
F32 = jnp.float32


def legendre_table(positions, points):
    columns = [positions * 0.0 + 1.0, positions]
    for degree_now in range(2, points):
        columns.append(
            ((2 * degree_now - 1) * positions * columns[-1] - (degree_now - 1) * columns[-2])
            / degree_now
        )
    return np.stack(columns, axis=1)


def gll_derivative(points):
    degree = points - 1
    grid_nodes = -np.cos(np.pi * np.arange(points) / degree)
    for _ in range(100):
        legendre = legendre_table(grid_nodes, points)
        grid_nodes = grid_nodes - (grid_nodes * legendre[:, degree] - legendre[:, degree - 1]) / (
            points * legendre[:, degree]
        )
    legendre = legendre_table(grid_nodes, points)
    top_values = legendre[:, degree]
    index_list = np.arange(points)
    same_index = index_list[:, None] == index_list[None, :]
    spacing = grid_nodes[:, None] - grid_nodes[None, :]
    spacing = np.where(same_index, 1.0, spacing)
    deriv_table = top_values[:, None] / (top_values[None, :] * spacing)
    deriv_table = np.where(same_index, 0.0, deriv_table)
    deriv_table[0, 0] = -degree * points / 4.0
    deriv_table[degree, degree] = degree * points / 4.0
    return deriv_table


DERIV = gll_derivative(NODES)
HALF_N = NODES // 2
MIRROR = DERIV[:, ::-1]
ON_SUM = 0.5 * (DERIV + MIRROR)[:HALF_N, :HALF_N]
ON_DIFF = 0.5 * (DERIV - MIRROR)[:HALF_N, :HALF_N]
SQUARED = DERIV * DERIV
SQ_SUM = 0.5 * (SQUARED + SQUARED[::-1])[:HALF_N, :HALF_N]
SQ_DIFF = 0.5 * (SQUARED - SQUARED[::-1])[:HALF_N, :HALF_N]

SIGMA = CENTRE / HALF
RHO_0 = 1.0 / SIGMA
RHO_1 = 1.0 / (2.0 * SIGMA - RHO_0)
KEEP = 1.0 + RHO_1 * RHO_0 + 2.0 * RHO_1 / HALF * CENTRE
PULL = -2.0 * RHO_1 / HALF


def combine(weights, values):
    total = None
    for weight, value in zip(weights, values):
        if weight == 0.0:
            continue
        term = value if weight == 1.0 else value * F32(weight)
        total = term if total is None else total + term
    return total


def fold(values):
    low, high = values[:HALF_N], values[: HALF_N - 1 : -1]
    return [a + b for a, b in zip(low, high)], [a - b for a, b in zip(low, high)]


def derive(values):
    even, odd = fold(values)
    by_even = [combine(ON_SUM[m], even) for m in range(HALF_N)]
    by_odd = [combine(ON_DIFF[m], odd) for m in range(HALF_N)]
    return [a + b for a, b in zip(by_even, by_odd)] + [
        b - a for a, b in zip(by_even[::-1], by_odd[::-1])
    ]


def derive_back(values):
    even, odd = fold(values)
    by_even = [combine(ON_DIFF[:, a], even) for a in range(HALF_N)]
    by_odd = [combine(ON_SUM[:, a], odd) for a in range(HALF_N)]
    return [a + b for a, b in zip(by_even, by_odd)] + [
        b - a for a, b in zip(by_even[::-1], by_odd[::-1])
    ]


def square_back(values):
    even, odd = fold(values)
    by_even = [combine(SQ_SUM[:, a], even) for a in range(HALF_N)]
    by_odd = [combine(SQ_DIFF[:, a], odd) for a in range(HALF_N)]
    return [a + b for a, b in zip(by_even, by_odd)] + [
        a - b for a, b in zip(by_even[::-1], by_odd[::-1])
    ]


def stiff_line(values, factors):
    return derive_back([g * d for g, d in zip(factors, derive(values))])


def lanes_of(value, index):
    return jnp.take_along_axis(value, index, axis=1, mode="promise_in_bounds")


class Shared:
    def __init__(self):
        lane = lax.broadcasted_iota(jnp.int32, (8, 128), 1)
        row = lax.broadcasted_iota(jnp.int32, (8, 128), 0)
        pos_z = lane % EL_Z
        up = lane - pos_z + (pos_z + 1) % EL_Z
        down = lane - pos_z + (pos_z + EL_Z - 1) % EL_Z
        self.across = jnp.where(row == 0, up, down)
        self.has_low = lane >= EL_Z
        self.has_high = lane < CELLS - EL_Z
        self.first = row == 0
        self.last = row == NODES - 1

    def plane(self, rows):
        low, high = rows[0], rows[-1]
        zero = jnp.zeros_like(low)
        new_low = low + jnp.where(self.has_low, pltpu.roll(high, EL_Z, 1), zero)
        new_high = high + jnp.where(self.has_high, pltpu.roll(low, CELLS - EL_Z, 1), zero)
        out = []
        for value in [new_low, *rows[1:-1], new_high]:
            moved = lanes_of(value, self.across)
            from_last = pltpu.roll(moved, 1, 0)
            from_first = pltpu.roll(moved, NODES - 1, 0)
            added = jnp.where(self.first, from_last, jnp.where(self.last, from_first, zero))
            out.append(value + added)
        return out


def rows_of(ref, *at):
    return [ref[(*at, pl.ds(8 * b, 8), slice(None))] for b in range(NODES)]


def put_rows(ref, values, *at):
    for b, value in enumerate(values):
        ref[(*at, pl.ds(8 * b, 8), slice(None))] = value


def turned(ref, *at):
    return [ref[(*at, pl.ds(c, 8, stride=8), slice(None))] for c in range(NODES)]


def mirrored():
    core = lax.axis_index("core")
    return [a + core * (NODES - 1 - 2 * a) for a in range(NODES)]


def prepare(order_in, load_in, geom_in, mass_in, load, geo_a, geo_b, geo_c, mass, diag, lead, message, order_ref, raw, work, index_ref, sems):
    order_copy = pltpu.make_async_copy(order_in, order_ref, sems.at[5])
    order_copy.start()
    sources = [geom_in.at[0], geom_in.at[1], geom_in.at[2], mass_in, load_in]
    copies = [pltpu.make_async_copy(src, raw.at[i], sems.at[i]) for i, src in enumerate(sources)]
    for copy in copies:
        copy.start()

    @pl.when(lax.axis_index("core") >= 0)
    def invert():
        order_copy.wait()
        cells = jnp.broadcast_to(order_ref[...], (CELLS, CELLS))
        hot = (cells == lax.broadcasted_iota(jnp.int32, (CELLS, CELLS), 0)).astype(F32)
        column = lax.broadcasted_iota(jnp.int32, (8, CELLS), 1).astype(F32)
        index = lax.dot_general(column, hot, (((1,), (1,)), ((), ())), preferred_element_type=F32)
        index_ref[...] = index.astype(jnp.int32)

    at = mirrored()
    for copy in copies:
        copy.wait()
    index = index_ref[...]

    def fetch(which, a):
        return [lanes_of(v, index) for v in rows_of(raw, which, at[a])]

    for b in range(NODES):
        here = pl.ds(8 * b, 8)
        lines = [lanes_of(raw[0, at[a], here, :], index) for a in range(NODES)]
        part = square_back(lines)
        for a in range(NODES):
            geo_a[a, here, :] = lines[a]
        lead[here, :] = part[0]
        for a in range(1, NODES - 1):
            diag[a, here, :] = part[a]
        message[1, here, :] = part[NODES - 1]
    for a in range(NODES):
        lines = [lanes_of(v, index) for v in turned(raw, 2, at[a])]
        put_rows(geo_c, lines, a)
        if 0 < a < NODES - 1:
            put_rows(work, square_back(lines), a)
        elif a == NODES - 1:
            put_rows(message, lines, 4)
    for a in range(NODES):
        lines, weights, values = fetch(1, a), fetch(3, a), fetch(4, a)
        put_rows(geo_b, lines, a)
        put_rows(mass, weights, a)
        put_rows(load, values, a)
        if a == 0:
            put_rows(lead, [x + y for x, y in zip(rows_of(lead), weights)])
        elif a == NODES - 1:
            for i, rows in ((0, values), (2, weights), (3, lines)):
                put_rows(message, rows, i)
        else:
            parts = square_back(lines), turned(work, a), weights, rows_of(diag, a)
            put_rows(diag, [w + x + y + z for w, x, y, z in zip(*parts)], a)


def summed(ref, which):
    return [x + y for x, y in zip(rows_of(ref, 0, which), rows_of(ref, 1, which))]


def settle(shared, load, lead, fac_b, fac_c, work):
    put_rows(work, square_back(fac_c))
    low = [x + y + z for x, y, z in zip(square_back(fac_b), turned(work), lead)]
    low = [1.0 / v for v in shared.plane(low)]
    top = shared.plane(load)
    return top, low, [x * y * F32(1.0 / CENTRE) for x, y in zip(top, low)]


def within(values, lead, fac_b, fac_c, keep, work):
    put_rows(keep, values)
    put_rows(work, stiff_line(turned(keep), fac_c))
    part = stiff_line(values, fac_b)
    return [k * u + x + y for k, u, x, y in zip(lead, values, part, turned(work))]


def begin(load, geo_a, geo_b, geo_c, diag, lead, pair, start, recip, first, slope, message, end, keep, work):
    shared = Shared()
    mass_7, fac_b, fac_c = summed(pair, 2), summed(pair, 3), summed(pair, 4)
    lead_7 = [x + y for x, y in zip(summed(pair, 1), mass_7)]
    top, low, tail = settle(shared, summed(pair, 0), lead_7, fac_b, fac_c, work)
    put_rows(start, top, NODES - 1)
    put_rows(recip, low, NODES - 1)
    put_rows(first, tail, NODES - 1)
    put_rows(end, lead_7, 0)
    put_rows(end, fac_b, 1)
    put_rows(end, fac_c, 2)
    put_rows(end, within(tail, mass_7, fac_b, fac_c, keep, work), 3)
    for a in range(1, NODES - 1):
        top, low = shared.plane(rows_of(load, a)), shared.plane(rows_of(diag, a))
        low = [1.0 / v for v in low]
        put_rows(start, top, a)
        put_rows(recip, low, a)
        put_rows(first, [x * y * F32(1.0 / CENTRE) for x, y in zip(top, low)], a)
    for b in range(NODES):
        here = pl.ds(8 * b, 8)
        zero = jnp.zeros((8, 128), F32)
        grad = derive([zero] + [first[a, here, :] for a in range(1, NODES)])
        for a in range(NODES):
            slope[a, here, :] = grad[a]
        flux = [geo_a[a, here, :] * grad[a] for a in range(NODES)]
        message[1, here, :] = combine(DERIV[:, 0], flux)
    put_rows(message, rows_of(load, 0), 0)
    put_rows(message, rows_of(lead), 2)
    put_rows(message, rows_of(geo_b, 0), 3)
    put_rows(message, rows_of(geo_c, 0), 4)


def improve(first, image, recip):
    return [u * F32(KEEP) + q * d * F32(PULL) for u, q, d in zip(first, image, recip)]


def middle(both, geo_a, geo_b, geo_c, mass, recip, first, slope, start0, precond, ahead, message, keep, local, work):
    shared = Shared()
    lead, fac_b, fac_c = summed(both, 2), summed(both, 3), summed(both, 4)
    top, low, head = settle(shared, summed(both, 0), lead, fac_b, fac_c, work.at[0])
    put_rows(start0, top)
    image = within(head, lead, fac_b, fac_c, keep, work.at[0])
    image = shared.plane([x + y for x, y in zip(summed(both, 1), image)])
    put_rows(precond, improve(head, image, low), 0)
    for b in range(NODES):
        here = pl.ds(8 * b, 8)
        flux = []
        for a in range(NODES):
            flux.append(geo_a[a, here, :] * (slope[a, here, :] + head[b] * F32(DERIV[a, 0])))
        back = derive_back(flux)
        for a in range(1, NODES - 1):
            local[a, here, :] = back[a]
        message[0, here, :] = back[NODES - 1]
    for a in range(1, NODES - 1):
        put_rows(work, stiff_line(turned(first, a), rows_of(geo_c, a)), a)
    for a in range(1, NODES - 1):
        values = rows_of(first, a)
        part = stiff_line(values, rows_of(geo_b, a))
        turn = turned(work, a)
        image = [
            x + y + z + m * v
            for x, y, z, m, v in zip(rows_of(local, a), part, turn, rows_of(mass, a), values)
        ]
        put_rows(precond, improve(values, shared.plane(image), rows_of(recip, a)), a)
    for b in range(NODES):
        here = pl.ds(8 * b, 8)
        zero = jnp.zeros((8, 128), F32)
        grad = derive([precond[a, here, :] for a in range(NODES - 1)] + [zero])
        for a in range(NODES):
            ahead[a, here, :] = grad[a]
        flux = [geo_a[a, here, :] * grad[a] for a in range(NODES)]
        message[1, here, :] = combine(DERIV[:, NODES - 1], flux)


def finish(pair, end, geo_a, geo_b, geo_c, mass, load, recip, first, precond_in, ahead, precond, image, outer, row, keep, flux_a, flux_b, flux_c, row_buf, row_sem):
    shared = Shared()
    whole = shared.plane([x + y for x, y in zip(summed(pair, 0), rows_of(end, 3))])
    tail = improve(rows_of(first, NODES - 1), whole, rows_of(recip, NODES - 1))
    put_rows(precond, tail)

    def iterate(a):
        return tail if a == NODES - 1 else rows_of(precond_in, a)

    over = [jnp.zeros((8, 128), F32) for _ in range(NODES)]
    under = [jnp.zeros((8, 128), F32) for _ in range(NODES)]
    for b in range(NODES):
        here = pl.ds(8 * b, 8)
        for a in range(NODES):
            grad = ahead[a, here, :] + tail[b] * F32(DERIV[a, NODES - 1])
            flux = geo_a[a, here, :] * grad
            flux_a[a, here, :] = flux
            under[a] = under[a] + flux * grad
    for a in range(NODES):
        grad = derive(turned(precond) if a == NODES - 1 else turned(precond_in, a))
        flux = [g * d for g, d in zip(rows_of(geo_c, a), grad)]
        put_rows(flux_c, flux, a)
        under = [s + f * d for s, f, d in zip(under, flux, grad)]
    for a in range(NODES):
        values = iterate(a)
        grad = derive(values)
        flux = [g * d for g, d in zip(rows_of(geo_b, a), grad)]
        put_rows(flux_b, flux, a)
        under = [s + f * d for s, f, d in zip(under, flux, grad)]
        under = [s + m * v * v for s, m, v in zip(under, rows_of(mass, a), values)]
        over = [s + f * v for s, f, v in zip(over, rows_of(load, a), values)]
    over = jnp.sum(functools.reduce(jnp.add, over), axis=0, keepdims=True)
    under = jnp.sum(functools.reduce(jnp.add, under), axis=0, keepdims=True)
    over = over + pltpu.roll(over, 64, 1)
    under = under + pltpu.roll(under, 64, 1)
    lane = lax.broadcasted_iota(jnp.int32, (1, 128), 1)
    row_buf[...] = jnp.broadcast_to(jnp.where(lane < 64, over, under), row_buf.shape)
    row_copy = pltpu.make_async_copy(row_buf, row, row_sem)
    row_copy.start()

    @pl.when(lax.axis_index("core") >= 0)
    def apply():
        for b in range(NODES):
            here = pl.ds(8 * b, 8)
            back = derive_back([flux_a[a, here, :] for a in range(NODES)])
            for a in range(NODES - 1):
                flux_a[a, here, :] = back[a]
        for a in range(NODES - 1):
            put_rows(flux_c, derive_back(rows_of(flux_c, a)), a)
        for a in range(NODES - 1):
            values = rows_of(precond_in, a)
            part = derive_back(rows_of(flux_b, a))
            turn = turned(flux_c, a)
            total = [
                x + y + z + m * v
                for x, y, z, m, v in zip(rows_of(flux_a, a), part, turn, rows_of(mass, a), values)
            ]
            if a == 0:
                put_rows(outer, total)
            else:
                put_rows(image, Shared().plane(total), a)
        inside = within(rows_of(precond), rows_of(end, 0), rows_of(end, 1), rows_of(end, 2), keep, flux_c.at[NODES - 1])
        inside = [x + y for x, y in zip(summed(pair, 1), inside)]
        put_rows(image, Shared().plane(inside), NODES - 1)

    row_copy.wait()


def restore(order_ref, start_in, start0, precond_in, last, image_in, start, precond, image):
    index = jnp.broadcast_to(order_ref[...], (8, CELLS))
    for a in range(NODES):
        for out, rows in (
            (start, rows_of(start0) if a == 0 else rows_of(start_in, a)),
            (precond, rows_of(last) if a == NODES - 1 else rows_of(precond_in, a)),
            (image, None if a == 0 else rows_of(image_in, a)),
        ):
            if rows is not None:
                put_rows(out, [lanes_of(v, index) for v in rows], a)


def step_length(sums, alpha):
    lane = lax.broadcasted_iota(jnp.int32, (1, 128), 1)
    total = jnp.sum(sums[...], axis=0, keepdims=True)
    zero = jnp.zeros_like(total)
    over = jnp.sum(jnp.where(lane < 64, total, zero), axis=1, keepdims=True)
    under = jnp.sum(jnp.where(lane < 64, zero, total), axis=1, keepdims=True)
    alpha[...] = jnp.broadcast_to(over / under, (8, 128))


def close(alpha_ref, order_ref, outer, outer_other, start, precond, image, solution_out, residual_out, buf_s, buf_r, sems):
    shared = Shared()
    alpha = alpha_ref[...]
    index = jnp.broadcast_to(order_ref[...], (8, CELLS))
    at = mirrored()
    head = shared.plane([x + y for x, y in zip(rows_of(outer), rows_of(outer_other))])
    head = [lanes_of(v, index) for v in head]
    copies = []
    for a in (1, 2, 3, 4, 5, 6, 7, 0):
        rows = head if a == 0 else rows_of(image, a)
        for b, (v, s, i) in enumerate(zip(rows_of(precond, a), rows_of(start, a), rows)):
            buf_s[a, b] = alpha * v
            buf_r[a, b] = s - alpha * i
        for i, (buf, out) in enumerate(((buf_s, solution_out), (buf_r, residual_out))):
            copy = pltpu.make_async_copy(buf.at[a], out.at[at[a]], sems.at[i, a])
            copy.start()
            copies.append(copy)
    for copy in copies:
        copy.wait()


def gather_up(sums, row):
    row[...] = jnp.broadcast_to(jnp.sum(sums[...], axis=0, keepdims=True), row.shape)


VMEM = pl.BlockSpec(memory_space=pltpu.VMEM)
HBM = pl.BlockSpec(memory_space=pltpu.HBM)
ANY = pl.BlockSpec(memory_space=pl.ANY)
FIELD = (NODES, 64, 128)
FACE = (64, 128)
BLOCK = (NODES, NODES, NODES, CELLS)


def call(body, outs, ins, scratch=(), out_specs=None, flops=4_000_000):
    return pl.pallas_call(
        body,
        out_shape=[jax.ShapeDtypeStruct(s, F32) if isinstance(s, tuple) else s for s in outs],
        in_specs=ins,
        out_specs=out_specs or [VMEM] * len(outs),
        scratch_shapes=list(scratch),
        compiler_params=pltpu.CompilerParams(vmem_limit_bytes=12 << 20),
        cost_estimate=pl.CostEstimate(flops=flops, bytes_accessed=2 << 20, transcendentals=0),
    )


def on_device(load_terms, geometry, mass_terms, element_order):
    count = 1
    for axis in AXES:
        count *= lax.axis_size(axis)
    across_chips = [[2 * k + 1, (2 * k + 2) % count] for k in range(count // 2)]
    first_groups, second_groups = groups((1, 3)), groups((0, 2))
    in_chip = [[2 * k + 1, 2 * k] for k in range(count // 2)]
    swap = [(i, (i + 1) % count if i % 2 else (i - 1) % count) for i in range(count)]
    dma = pltpu.SemaphoreType.DMA
    arguments = (
        element_order,
        load_terms.reshape(FIELD),
        geometry.reshape(3, *FIELD),
        mass_terms.reshape(FIELD),
    )
    arguments = [pltpu.with_memory_space_constraint(x, pltpu.HBM) for x in arguments]

    load, geo_a, geo_b, geo_c, mass, diag, lead, message, order = call(
        prepare,
        [FIELD] * 6 + [FACE, (5, *FACE), jax.ShapeDtypeStruct((1, CELLS), jnp.int32)],
        [HBM] * 4,
        [
            pltpu.VMEM((5, *FIELD), F32),
            pltpu.VMEM(FIELD, F32),
            pltpu.VMEM((8, CELLS), jnp.int32),
            dma((6,)),
        ],
    )(*arguments)
    pair = lax.all_gather(message, AXES, axis_index_groups=in_chip)
    start, recip, first, slope, message, end = call(
        begin, [FIELD] * 4 + [(5, *FACE), (4, *FACE)], [VMEM] * 7, [pltpu.VMEM(FACE, F32), pltpu.VMEM(FACE, F32)]
    )(load, geo_a, geo_b, geo_c, diag, lead, pair)
    both = lax.all_gather(message, AXES, axis_index_groups=across_chips)
    start0, precond, ahead, message = call(
        middle,
        [FACE, FIELD, FIELD, (2, *FACE)],
        [VMEM] * 8,
        [pltpu.VMEM(FACE, F32), pltpu.VMEM(FIELD, F32), pltpu.VMEM(FIELD, F32)],
    )(both, geo_a, geo_b, geo_c, mass, recip, first, slope)
    pair = lax.all_gather(message, AXES, axis_index_groups=in_chip)
    last, image, outer, row = call(
        finish,
        [FACE, FIELD, FACE, (len(first_groups[0]), 128)],
        [VMEM] * 11,
        [
            pltpu.VMEM(FACE, F32),
            *[pltpu.VMEM(FIELD, F32)] * 3,
            pltpu.VMEM((len(first_groups[0]), 128), F32),
            dma,
        ],
        out_specs=[VMEM] * 3 + [ANY],
    )(pair, end, geo_a, geo_b, geo_c, mass, load, recip, first, precond, ahead)
    outer_other = lax.ppermute(outer, AXES, swap)
    sums = lax.all_to_all(row, AXES, 0, 0, tiled=True, axis_index_groups=first_groups)
    (row,) = call(gather_up, [(len(second_groups[0]), 128)], [VMEM], flops=100_000)(sums)
    sums = lax.all_to_all(row, AXES, 0, 0, tiled=True, axis_index_groups=second_groups)
    (alpha,) = call(step_length, [(8, 128)], [VMEM], flops=100_000)(sums)
    start, precond, image = call(restore, [FIELD] * 3, [VMEM] * 6)(order, start, start0, precond, last, image)
    solution, residual = call(
        close,
        [BLOCK, BLOCK],
        [VMEM] * 7,
        [pltpu.VMEM(BLOCK, F32), pltpu.VMEM(BLOCK, F32), dma((2, NODES))],
        out_specs=[ANY, ANY],
    )(alpha, order, outer, outer_other, start, precond, image)
    return solution, residual


def solution(mesh):
    torus = Mesh(mesh.devices.reshape(TORUS), AXES)
    placed = (
        P(None, None, None, AXES),
        P(None, None, None, None, AXES),
        P(None, None, None, AXES),
        P(AXES, None),
    )
    return jax.shard_map(
        on_device,
        mesh=torus,
        in_specs=placed,
        out_specs=(P(None, None, None, AXES), P(None, None, None, AXES)),
        check_vma=False,
    )
```

```python
import functools

import jax
import jax.numpy as jnp
import numpy as np
from jax import lax
from jax.experimental import pallas as pl
from jax.experimental.pallas import tpu as pltpu
from jax.sharding import Mesh
from jax.sharding import PartitionSpec as P


TORUS = (8, 12, 4, 2)
AXES = ("ty", "tz", "tx", "core")
LINE_ROOT = (10, 10, 10, 9)
PLANE_ROOT = (5, 3)


def groups(axes):
    ids = np.arange(np.prod(TORUS)).reshape(TORUS)
    out = []
    if axes == (1, 3):
        for y in range(TORUS[0]):
            for x in range(TORUS[2]):
                z = LINE_ROOT[x]
                out.append(np.roll(ids[y, :, x, :], [-z, -1], (0, 1)).reshape(-1).tolist())
        return out
    for z in range(TORUS[1]):
        for c in range(TORUS[3]):
            out.append(np.roll(ids[:, z, :, c], [-PLANE_ROOT[0], -PLANE_ROOT[1]], (0, 1)).reshape(-1).tolist())
    return out


NODES = 8
EL_Y = 8
EL_Z = 16
CELLS = EL_Y * EL_Z
CENTRE = 1.65
HALF = 1.35
F32 = jnp.float32


def legendre_table(positions, points):
    columns = [positions * 0.0 + 1.0, positions]
    for degree_now in range(2, points):
        columns.append(
            ((2 * degree_now - 1) * positions * columns[-1] - (degree_now - 1) * columns[-2])
            / degree_now
        )
    return np.stack(columns, axis=1)


def gll_derivative(points):
    degree = points - 1
    grid_nodes = -np.cos(np.pi * np.arange(points) / degree)
    for _ in range(100):
        legendre = legendre_table(grid_nodes, points)
        grid_nodes = grid_nodes - (grid_nodes * legendre[:, degree] - legendre[:, degree - 1]) / (
            points * legendre[:, degree]
        )
    legendre = legendre_table(grid_nodes, points)
    top_values = legendre[:, degree]
    index_list = np.arange(points)
    same_index = index_list[:, None] == index_list[None, :]
    spacing = grid_nodes[:, None] - grid_nodes[None, :]
    spacing = np.where(same_index, 1.0, spacing)
    deriv_table = top_values[:, None] / (top_values[None, :] * spacing)
    deriv_table = np.where(same_index, 0.0, deriv_table)
    deriv_table[0, 0] = -degree * points / 4.0
    deriv_table[degree, degree] = degree * points / 4.0
    return deriv_table


DERIV = gll_derivative(NODES)
HALF_N = NODES // 2
MIRROR = DERIV[:, ::-1]
ON_SUM = 0.5 * (DERIV + MIRROR)[:HALF_N, :HALF_N]
ON_DIFF = 0.5 * (DERIV - MIRROR)[:HALF_N, :HALF_N]
SQUARED = DERIV * DERIV
SQ_SUM = 0.5 * (SQUARED + SQUARED[::-1])[:HALF_N, :HALF_N]
SQ_DIFF = 0.5 * (SQUARED - SQUARED[::-1])[:HALF_N, :HALF_N]

SIGMA = CENTRE / HALF
RHO_0 = 1.0 / SIGMA
RHO_1 = 1.0 / (2.0 * SIGMA - RHO_0)
KEEP = 1.0 + RHO_1 * RHO_0 + 2.0 * RHO_1 / HALF * CENTRE
PULL = -2.0 * RHO_1 / HALF


def combine(weights, values):
    total = None
    for weight, value in zip(weights, values):
        if weight == 0.0:
            continue
        term = value if weight == 1.0 else value * F32(weight)
        total = term if total is None else total + term
    return total


def fold(values):
    low, high = values[:HALF_N], values[: HALF_N - 1 : -1]
    return [a + b for a, b in zip(low, high)], [a - b for a, b in zip(low, high)]


def derive(values):
    even, odd = fold(values)
    by_even = [combine(ON_SUM[m], even) for m in range(HALF_N)]
    by_odd = [combine(ON_DIFF[m], odd) for m in range(HALF_N)]
    return [a + b for a, b in zip(by_even, by_odd)] + [
        b - a for a, b in zip(by_even[::-1], by_odd[::-1])
    ]


def derive_back(values):
    even, odd = fold(values)
    by_even = [combine(ON_DIFF[:, a], even) for a in range(HALF_N)]
    by_odd = [combine(ON_SUM[:, a], odd) for a in range(HALF_N)]
    return [a + b for a, b in zip(by_even, by_odd)] + [
        b - a for a, b in zip(by_even[::-1], by_odd[::-1])
    ]


def square_back(values):
    even, odd = fold(values)
    by_even = [combine(SQ_SUM[:, a], even) for a in range(HALF_N)]
    by_odd = [combine(SQ_DIFF[:, a], odd) for a in range(HALF_N)]
    return [a + b for a, b in zip(by_even, by_odd)] + [
        a - b for a, b in zip(by_even[::-1], by_odd[::-1])
    ]


def stiff_line(values, factors):
    return derive_back([g * d for g, d in zip(factors, derive(values))])


def lanes_of(value, index):
    return jnp.take_along_axis(value, index, axis=1, mode="promise_in_bounds")


class Shared:
    def __init__(self):
        lane = lax.broadcasted_iota(jnp.int32, (8, 128), 1)
        row = lax.broadcasted_iota(jnp.int32, (8, 128), 0)
        pos_z = lane % EL_Z
        up = lane - pos_z + (pos_z + 1) % EL_Z
        down = lane - pos_z + (pos_z + EL_Z - 1) % EL_Z
        self.across = jnp.where(row == 0, up, down)
        self.has_low = lane >= EL_Z
        self.has_high = lane < CELLS - EL_Z
        self.first = row == 0
        self.last = row == NODES - 1
        self.front = pos_z == 0
        self.back = pos_z == EL_Z - 1

    def plane(self, rows):
        low, high = rows[0], rows[-1]
        zero = jnp.zeros_like(low)
        new_low = low + jnp.where(self.has_low, pltpu.roll(high, EL_Z, 1), zero)
        new_high = high + jnp.where(self.has_high, pltpu.roll(low, CELLS - EL_Z, 1), zero)
        out = []
        for value in [new_low, *rows[1:-1], new_high]:
            moved = lanes_of(value, self.across)
            from_last = pltpu.roll(moved, 1, 0)
            from_first = pltpu.roll(moved, NODES - 1, 0)
            added = jnp.where(self.first, from_last, jnp.where(self.last, from_first, zero))
            out.append(value + added)
        return out


def share(shared, ref, a, rows):
    low, high = rows[0], rows[-1]
    zero = jnp.zeros_like(low)
    new_low = low + jnp.where(shared.has_low, pltpu.roll(high, EL_Z, 1), zero)
    new_high = high + jnp.where(shared.has_high, pltpu.roll(low, CELLS - EL_Z, 1), zero)
    put_rows(ref, [new_low, *rows[1:-1], new_high], a)
    near, far = pl.ds(0, NODES, stride=8), pl.ds(NODES - 1, NODES, stride=8)
    first, last = ref[a, near, :], ref[a, far, :]
    before = jnp.where(shared.front, pltpu.roll(last, CELLS - EL_Z + 1, 1), pltpu.roll(last, 1, 1))
    after = jnp.where(shared.back, pltpu.roll(first, EL_Z - 1, 1), pltpu.roll(first, CELLS - 1, 1))
    ref[a, near, :] = first + before
    ref[a, far, :] = last + after


def rows_of(ref, *at):
    return [ref[(*at, pl.ds(8 * b, 8), slice(None))] for b in range(NODES)]


def put_rows(ref, values, *at):
    for b, value in enumerate(values):
        ref[(*at, pl.ds(8 * b, 8), slice(None))] = value


def turned(ref, *at):
    return [ref[(*at, pl.ds(c, 8, stride=8), slice(None))] for c in range(NODES)]


def mirrored():
    core = lax.axis_index("core")
    return [a + core * (NODES - 1 - 2 * a) for a in range(NODES)]


def prepare(order_in, load_in, geom_in, mass_in, load, geo_a, geo_b, geo_c, mass, diag, lead, message, order_ref, raw, work, index_ref, sems):
    order_copy = pltpu.make_async_copy(order_in, order_ref, sems.at[5])
    order_copy.start()
    sources = [geom_in.at[0], geom_in.at[1], geom_in.at[2], mass_in, load_in]
    copies = [pltpu.make_async_copy(src, raw.at[i], sems.at[i]) for i, src in enumerate(sources)]
    for copy in copies:
        copy.start()

    @pl.when(lax.axis_index("core") >= 0)
    def invert():
        order_copy.wait()
        cells = jnp.broadcast_to(order_ref[...], (CELLS, CELLS))
        hot = (cells == lax.broadcasted_iota(jnp.int32, (CELLS, CELLS), 0)).astype(F32)
        column = lax.broadcasted_iota(jnp.int32, (8, CELLS), 1).astype(F32)
        index = lax.dot_general(column, hot, (((1,), (1,)), ((), ())), preferred_element_type=F32)
        index_ref[...] = index.astype(jnp.int32)

    at = mirrored()
    for copy in copies[:3]:
        copy.wait()
    index = index_ref[...]

    def fetch(which, a):
        return [lanes_of(v, index) for v in rows_of(raw, which, at[a])]

    for b in range(NODES):
        here = pl.ds(8 * b, 8)
        lines = [lanes_of(raw[0, at[a], here, :], index) for a in range(NODES)]
        part = square_back(lines)
        for a in range(NODES):
            geo_a[a, here, :] = lines[a]
        lead[here, :] = part[0]
        for a in range(1, NODES - 1):
            diag[a, here, :] = part[a]
        message[1, here, :] = part[NODES - 1]
    for a in range(NODES):
        lines = [lanes_of(v, index) for v in turned(raw, 2, at[a])]
        put_rows(geo_c, lines, a)
        if 0 < a < NODES - 1:
            put_rows(work, square_back(lines), a)
        elif a == NODES - 1:
            put_rows(message, lines, 4)
    for copy in copies[3:]:
        copy.wait()
    for a in range(NODES):
        lines, weights, values = fetch(1, a), fetch(3, a), fetch(4, a)
        put_rows(geo_b, lines, a)
        put_rows(mass, weights, a)
        put_rows(load, values, a)
        if a == 0:
            put_rows(lead, [x + y for x, y in zip(rows_of(lead), weights)])
        elif a == NODES - 1:
            for i, rows in ((0, values), (2, weights), (3, lines)):
                put_rows(message, rows, i)
        else:
            parts = square_back(lines), turned(work, a), weights, rows_of(diag, a)
            put_rows(diag, [w + x + y + z for w, x, y, z in zip(*parts)], a)


def summed(ref, which):
    return [x + y for x, y in zip(rows_of(ref, 0, which), rows_of(ref, 1, which))]


def settle(shared, load, lead, fac_b, fac_c, work):
    put_rows(work, square_back(fac_c))
    low = [x + y + z for x, y, z in zip(square_back(fac_b), turned(work), lead)]
    low = [1.0 / v for v in shared.plane(low)]
    top = shared.plane(load)
    return top, low, [x * y * F32(1.0 / CENTRE) for x, y in zip(top, low)]


def within(values, lead, fac_b, fac_c, keep, work):
    put_rows(keep, values)
    put_rows(work, stiff_line(turned(keep), fac_c))
    part = stiff_line(values, fac_b)
    return [k * u + x + y for k, u, x, y in zip(lead, values, part, turned(work))]


def begin(load, geo_a, geo_b, geo_c, diag, lead, pair, start, recip, first, slope, message, end, keep, work):
    shared = Shared()
    mass_7, fac_b, fac_c = summed(pair, 2), summed(pair, 3), summed(pair, 4)
    lead_7 = [x + y for x, y in zip(summed(pair, 1), mass_7)]
    top, low, tail = settle(shared, summed(pair, 0), lead_7, fac_b, fac_c, work)
    put_rows(start, top, NODES - 1)
    put_rows(recip, low, NODES - 1)
    put_rows(first, tail, NODES - 1)
    put_rows(end, lead_7, 0)
    put_rows(end, fac_b, 1)
    put_rows(end, fac_c, 2)
    put_rows(end, mass_7, 3)
    for a in range(1, NODES - 1):
        share(shared, start, a, rows_of(load, a))
        share(shared, recip, a, rows_of(diag, a))
    for a in range(1, NODES - 1):
        top, low = rows_of(start, a), [1.0 / v for v in rows_of(recip, a)]
        put_rows(recip, low, a)
        put_rows(first, [x * y * F32(1.0 / CENTRE) for x, y in zip(top, low)], a)
    for b in range(NODES):
        here = pl.ds(8 * b, 8)
        zero = jnp.zeros((8, 128), F32)
        grad = derive([zero] + [first[a, here, :] for a in range(1, NODES)])
        for a in range(NODES):
            slope[a, here, :] = grad[a]
        flux = [geo_a[a, here, :] * grad[a] for a in range(NODES)]
        message[1, here, :] = combine(DERIV[:, 0], flux)
    put_rows(message, rows_of(load, 0), 0)
    put_rows(message, rows_of(lead), 2)
    put_rows(message, rows_of(geo_b, 0), 3)
    put_rows(message, rows_of(geo_c, 0), 4)

    @pl.when(lax.axis_index("core") == 0)
    def inner():
        tail = rows_of(first, NODES - 1)
        put_rows(end, within(tail, rows_of(end, 3), rows_of(end, 1), rows_of(end, 2), keep, work), 3)


def improve(first, image, recip):
    return [u * F32(KEEP) + q * d * F32(PULL) for u, q, d in zip(first, image, recip)]


def middle(both, end, geo_a, geo_b, geo_c, mass, recip, first, slope, start0, precond, ahead, message, keep, local, work):
    shared = Shared()
    once = (1 - lax.axis_index("core")).astype(F32)
    lead, fac_b, fac_c = summed(both, 2), summed(both, 3), summed(both, 4)
    top, low, head = settle(shared, summed(both, 0), lead, fac_b, fac_c, work.at[0])
    put_rows(start0, top)
    image = within(head, lead, fac_b, fac_c, keep, work.at[0])
    image = shared.plane([x + y for x, y in zip(summed(both, 1), image)])
    put_rows(precond, improve(head, image, low), 0)
    for b in range(NODES):
        here = pl.ds(8 * b, 8)
        flux = []
        for a in range(NODES):
            flux.append(geo_a[a, here, :] * (slope[a, here, :] + head[b] * F32(DERIV[a, 0])))
        back = derive_back(flux)
        for a in range(1, NODES - 1):
            local[a, here, :] = back[a]
        message[0, here, :] = back[NODES - 1] + end[3, here, :] * once
    for a in range(1, NODES - 1):
        put_rows(work, stiff_line(turned(first, a), rows_of(geo_c, a)), a)
    for a in range(1, NODES - 1):
        values = rows_of(first, a)
        part = stiff_line(values, rows_of(geo_b, a))
        turn = turned(work, a)
        image = [
            x + y + z + m * v
            for x, y, z, m, v in zip(rows_of(local, a), part, turn, rows_of(mass, a), values)
        ]
        put_rows(precond, improve(values, shared.plane(image), rows_of(recip, a)), a)
    for b in range(NODES):
        here = pl.ds(8 * b, 8)
        zero = jnp.zeros((8, 128), F32)
        grad = derive([precond[a, here, :] for a in range(NODES - 1)] + [zero])
        for a in range(NODES):
            ahead[a, here, :] = grad[a]
        flux = [geo_a[a, here, :] * grad[a] for a in range(NODES)]
        message[1, here, :] = combine(DERIV[:, NODES - 1], flux)


def finish(pair, end, geo_a, geo_b, geo_c, mass, load, recip, first, precond_in, ahead, precond, image, outer, row, keep, flux_a, flux_b, flux_c, row_buf, row_sem):
    shared = Shared()
    whole = shared.plane(summed(pair, 0))
    tail = improve(rows_of(first, NODES - 1), whole, rows_of(recip, NODES - 1))
    put_rows(precond, tail)

    def iterate(a):
        return tail if a == NODES - 1 else rows_of(precond_in, a)

    over = [jnp.zeros((8, 128), F32) for _ in range(NODES)]
    under = [jnp.zeros((8, 128), F32) for _ in range(NODES)]
    for b in range(NODES):
        here = pl.ds(8 * b, 8)
        for a in range(NODES):
            grad = ahead[a, here, :] + tail[b] * F32(DERIV[a, NODES - 1])
            flux = geo_a[a, here, :] * grad
            flux_a[a, here, :] = flux
            under[a] = under[a] + flux * grad
    for a in range(NODES):
        grad = derive(turned(precond) if a == NODES - 1 else turned(precond_in, a))
        flux = [g * d for g, d in zip(rows_of(geo_c, a), grad)]
        put_rows(flux_c, flux, a)
        under = [s + f * d for s, f, d in zip(under, flux, grad)]
    for a in range(NODES):
        values = iterate(a)
        grad = derive(values)
        flux = [g * d for g, d in zip(rows_of(geo_b, a), grad)]
        put_rows(flux_b, flux, a)
        under = [s + f * d for s, f, d in zip(under, flux, grad)]
        under = [s + m * v * v for s, m, v in zip(under, rows_of(mass, a), values)]
        over = [s + f * v for s, f, v in zip(over, rows_of(load, a), values)]
    over = jnp.sum(functools.reduce(jnp.add, over), axis=0, keepdims=True)
    under = jnp.sum(functools.reduce(jnp.add, under), axis=0, keepdims=True)
    over = over + pltpu.roll(over, 64, 1)
    under = under + pltpu.roll(under, 64, 1)
    lane = lax.broadcasted_iota(jnp.int32, (1, 128), 1)
    row_buf[...] = jnp.broadcast_to(jnp.where(lane < 64, over, under), row_buf.shape)
    row_copy = pltpu.make_async_copy(row_buf, row, row_sem)
    row_copy.start()

    @pl.when(lax.axis_index("core") >= 0)
    def apply():
        for b in range(NODES):
            here = pl.ds(8 * b, 8)
            back = derive_back([flux_a[a, here, :] for a in range(NODES)])
            for a in range(NODES - 1):
                flux_a[a, here, :] = back[a]
        for a in range(NODES - 1):
            put_rows(flux_c, derive_back(rows_of(flux_c, a)), a)
        for a in range(NODES - 1):
            values = rows_of(precond_in, a)
            part = derive_back(rows_of(flux_b, a))
            turn = turned(flux_c, a)
            total = [
                x + y + z + m * v
                for x, y, z, m, v in zip(rows_of(flux_a, a), part, turn, rows_of(mass, a), values)
            ]
            if a == 0:
                put_rows(outer, Shared().plane(total))
            else:
                put_rows(image, Shared().plane(total), a)
        inside = within(rows_of(precond), rows_of(end, 0), rows_of(end, 1), rows_of(end, 2), keep, flux_c.at[NODES - 1])
        inside = [x + y for x, y in zip(summed(pair, 1), inside)]
        put_rows(image, Shared().plane(inside), NODES - 1)

    row_copy.wait()


def restore(order_ref, start_in, start0, precond_in, last, image_in, outer, start, precond, image):
    index = jnp.broadcast_to(order_ref[...], (8, CELLS))
    for a in range(NODES):
        for out, rows in (
            (start, rows_of(start0) if a == 0 else rows_of(start_in, a)),
            (precond, rows_of(last) if a == NODES - 1 else rows_of(precond_in, a)),
            (image, rows_of(outer) if a == 0 else rows_of(image_in, a)),
        ):
            put_rows(out, [lanes_of(v, index) for v in rows], a)


def step_length(sums, alpha):
    lane = lax.broadcasted_iota(jnp.int32, (1, 128), 1)
    total = jnp.sum(sums[...], axis=0, keepdims=True)
    zero = jnp.zeros_like(total)
    over = jnp.sum(jnp.where(lane < 64, total, zero), axis=1, keepdims=True)
    under = jnp.sum(jnp.where(lane < 64, zero, total), axis=1, keepdims=True)
    alpha[...] = jnp.broadcast_to(over / under, (8, 128))


def close(alpha_ref, order_ref, other, start, precond, image, solution_out, residual_out, buf_s, buf_r, sems):
    alpha = alpha_ref[...]
    index = jnp.broadcast_to(order_ref[...], (8, CELLS))
    at = mirrored()
    other = [lanes_of(v, index) for v in rows_of(other)]
    copies = []

    def send(i, a):
        buf, out = ((buf_s, solution_out), (buf_r, residual_out))[i]
        copies.append(pltpu.make_async_copy(buf.at[a], out.at[at[a]], sems.at[i, a]))
        copies[-1].start()

    for a in (1, 2, 3, 4, 5, 6, 7, 0):
        for b, v in enumerate(rows_of(precond, a)):
            buf_s[a, b] = alpha * v
        send(0, a)
        rows = rows_of(image, a)
        if a == 0:
            rows = [x + y for x, y in zip(rows, other)]
        for b, (s, i) in enumerate(zip(rows_of(start, a), rows)):
            buf_r[a, b] = s - alpha * i
        send(1, a)
    for copy in copies:
        copy.wait()


def gather_up(sums, row):
    row[...] = jnp.broadcast_to(jnp.sum(sums[...], axis=0, keepdims=True), row.shape)


VMEM = pl.BlockSpec(memory_space=pltpu.VMEM)
HBM = pl.BlockSpec(memory_space=pltpu.HBM)
ANY = pl.BlockSpec(memory_space=pl.ANY)
FIELD = (NODES, 64, 128)
FACE = (64, 128)
BLOCK = (NODES, NODES, NODES, CELLS)


def call(body, outs, ins, scratch=(), out_specs=None, flops=4_000_000):
    return pl.pallas_call(
        body,
        out_shape=[jax.ShapeDtypeStruct(s, F32) if isinstance(s, tuple) else s for s in outs],
        in_specs=ins,
        out_specs=out_specs or [VMEM] * len(outs),
        scratch_shapes=list(scratch),
        compiler_params=pltpu.CompilerParams(vmem_limit_bytes=12 << 20),
        cost_estimate=pl.CostEstimate(flops=flops, bytes_accessed=2 << 20, transcendentals=0),
    )


def on_device(load_terms, geometry, mass_terms, element_order):
    count = 1
    for axis in AXES:
        count *= lax.axis_size(axis)
    across_chips = [[2 * k + 1, (2 * k + 2) % count] for k in range(count // 2)]
    first_groups, second_groups = groups((1, 3)), groups((0, 2))
    in_chip = [[2 * k + 1, 2 * k] for k in range(count // 2)]
    swap = [(i, (i + 1) % count if i % 2 else (i - 1) % count) for i in range(count)]
    dma = pltpu.SemaphoreType.DMA
    arguments = (
        element_order,
        load_terms.reshape(FIELD),
        geometry.reshape(3, *FIELD),
        mass_terms.reshape(FIELD),
    )
    arguments = [pltpu.with_memory_space_constraint(x, pltpu.HBM) for x in arguments]

    load, geo_a, geo_b, geo_c, mass, diag, lead, message, order = call(
        prepare,
        [FIELD] * 6 + [FACE, (5, *FACE), jax.ShapeDtypeStruct((1, CELLS), jnp.int32)],
        [HBM] * 4,
        [
            pltpu.VMEM((5, *FIELD), F32),
            pltpu.VMEM(FIELD, F32),
            pltpu.VMEM((8, CELLS), jnp.int32),
            dma((6,)),
        ],
    )(*arguments)
    pair = lax.all_gather(message, AXES, axis_index_groups=in_chip)
    start, recip, first, slope, message, end = call(
        begin, [FIELD] * 4 + [(5, *FACE), (4, *FACE)], [VMEM] * 7, [pltpu.VMEM(FACE, F32), pltpu.VMEM(FACE, F32)]
    )(load, geo_a, geo_b, geo_c, diag, lead, pair)
    both = lax.all_gather(message, AXES, axis_index_groups=across_chips)
    start0, precond, ahead, message = call(
        middle,
        [FACE, FIELD, FIELD, (2, *FACE)],
        [VMEM] * 9,
        [pltpu.VMEM(FACE, F32), pltpu.VMEM(FIELD, F32), pltpu.VMEM(FIELD, F32)],
    )(both, end, geo_a, geo_b, geo_c, mass, recip, first, slope)
    pair = lax.all_gather(message, AXES, axis_index_groups=in_chip)
    last, image, outer, row = call(
        finish,
        [FACE, FIELD, FACE, (len(first_groups[0]), 128)],
        [VMEM] * 11,
        [
            pltpu.VMEM(FACE, F32),
            *[pltpu.VMEM(FIELD, F32)] * 3,
            pltpu.VMEM((len(first_groups[0]), 128), F32),
            dma,
        ],
        out_specs=[VMEM] * 3 + [ANY],
    )(pair, end, geo_a, geo_b, geo_c, mass, load, recip, first, precond, ahead)
    outer_other = lax.ppermute(outer, AXES, swap)
    sums = lax.all_to_all(row, AXES, 0, 0, tiled=True, axis_index_groups=first_groups)
    (row,) = call(gather_up, [(len(second_groups[0]), 128)], [VMEM], flops=100_000)(sums)
    sums = lax.all_to_all(row, AXES, 0, 0, tiled=True, axis_index_groups=second_groups)
    (alpha,) = call(step_length, [(8, 128)], [VMEM], flops=100_000)(sums)
    start, precond, image = call(restore, [FIELD] * 3, [VMEM] * 7)(order, start, start0, precond, last, image, outer)
    solution, residual = call(
        close,
        [BLOCK, BLOCK],
        [VMEM] * 6,
        [pltpu.VMEM(BLOCK, F32), pltpu.VMEM(BLOCK, F32), dma((2, NODES))],
        out_specs=[ANY, ANY],
    )(alpha, order, outer_other, start, precond, image)
    return solution, residual


def solution(mesh):
    torus = Mesh(mesh.devices.reshape(TORUS), AXES)
    placed = (
        P(None, None, None, AXES),
        P(None, None, None, None, AXES),
        P(None, None, None, AXES),
        P(AXES, None),
    )
    return jax.shard_map(
        on_device,
        mesh=torus,
        in_specs=placed,
        out_specs=(P(None, None, None, AXES), P(None, None, None, AXES)),
        check_vma=False,
    )
```

```python
import functools

import jax
import jax.numpy as jnp
import numpy as np
from jax import lax
from jax.experimental import pallas as pl
from jax.experimental.pallas import tpu as pltpu
from jax.sharding import Mesh
from jax.sharding import PartitionSpec as P


TORUS = (8, 12, 4, 2)
AXES = ("ty", "tz", "tx", "core")
LINE_ROOT = (10, 10, 10, 9)
PLANE_ROOT = (5, 3)


def groups(axes):
    ids = np.arange(np.prod(TORUS)).reshape(TORUS)
    out = []
    if axes == (1, 3):
        for y in range(TORUS[0]):
            for x in range(TORUS[2]):
                z = LINE_ROOT[x]
                out.append(np.roll(ids[y, :, x, :], [-z, -1], (0, 1)).reshape(-1).tolist())
        return out
    for z in range(TORUS[1]):
        for c in range(TORUS[3]):
            out.append(np.roll(ids[:, z, :, c], [-PLANE_ROOT[0], -PLANE_ROOT[1]], (0, 1)).reshape(-1).tolist())
    return out


NODES = 8
EL_Y = 8
EL_Z = 16
CELLS = EL_Y * EL_Z
CENTRE = 1.65
HALF = 1.35
F32 = jnp.float32


def legendre_table(positions, points):
    columns = [positions * 0.0 + 1.0, positions]
    for degree_now in range(2, points):
        columns.append(
            ((2 * degree_now - 1) * positions * columns[-1] - (degree_now - 1) * columns[-2])
            / degree_now
        )
    return np.stack(columns, axis=1)


def gll_derivative(points):
    degree = points - 1
    grid_nodes = -np.cos(np.pi * np.arange(points) / degree)
    for _ in range(100):
        legendre = legendre_table(grid_nodes, points)
        grid_nodes = grid_nodes - (grid_nodes * legendre[:, degree] - legendre[:, degree - 1]) / (
            points * legendre[:, degree]
        )
    legendre = legendre_table(grid_nodes, points)
    top_values = legendre[:, degree]
    index_list = np.arange(points)
    same_index = index_list[:, None] == index_list[None, :]
    spacing = grid_nodes[:, None] - grid_nodes[None, :]
    spacing = np.where(same_index, 1.0, spacing)
    deriv_table = top_values[:, None] / (top_values[None, :] * spacing)
    deriv_table = np.where(same_index, 0.0, deriv_table)
    deriv_table[0, 0] = -degree * points / 4.0
    deriv_table[degree, degree] = degree * points / 4.0
    return deriv_table


DERIV = gll_derivative(NODES)
HALF_N = NODES // 2
MIRROR = DERIV[:, ::-1]
ON_SUM = 0.5 * (DERIV + MIRROR)[:HALF_N, :HALF_N]
ON_DIFF = 0.5 * (DERIV - MIRROR)[:HALF_N, :HALF_N]
SQUARED = DERIV * DERIV
SQ_SUM = 0.5 * (SQUARED + SQUARED[::-1])[:HALF_N, :HALF_N]
SQ_DIFF = 0.5 * (SQUARED - SQUARED[::-1])[:HALF_N, :HALF_N]

SIGMA = CENTRE / HALF
RHO_0 = 1.0 / SIGMA
RHO_1 = 1.0 / (2.0 * SIGMA - RHO_0)
KEEP = 1.0 + RHO_1 * RHO_0 + 2.0 * RHO_1 / HALF * CENTRE
PULL = -2.0 * RHO_1 / HALF


def combine(weights, values):
    total = None
    for weight, value in zip(weights, values):
        if weight == 0.0:
            continue
        term = value if weight == 1.0 else value * F32(weight)
        total = term if total is None else total + term
    return total


def fold(values):
    low, high = values[:HALF_N], values[: HALF_N - 1 : -1]
    return [a + b for a, b in zip(low, high)], [a - b for a, b in zip(low, high)]


def derive(values):
    even, odd = fold(values)
    even = [v - even[-1] for v in even[:-1]]
    by_even = [combine(ON_SUM[m, :-1], even) for m in range(HALF_N)]
    by_odd = [combine(ON_DIFF[m], odd) for m in range(HALF_N)]
    return [a + b for a, b in zip(by_even, by_odd)] + [
        b - a for a, b in zip(by_even[::-1], by_odd[::-1])
    ]


def derive_back(values):
    even, odd = fold(values)
    by_even = [combine(ON_DIFF[:, a], even) for a in range(HALF_N)]
    by_odd = [combine(ON_SUM[:, a], odd) for a in range(HALF_N - 1)]
    by_odd.append(-(by_odd[0] + by_odd[1] + by_odd[2]))
    return [a + b for a, b in zip(by_even, by_odd)] + [
        b - a for a, b in zip(by_even[::-1], by_odd[::-1])
    ]


def square_back(values):
    even, odd = fold(values)
    by_even = [combine(SQ_SUM[:, a], even) for a in range(HALF_N)]
    by_odd = [combine(SQ_DIFF[:, a], odd) for a in range(HALF_N)]
    return [a + b for a, b in zip(by_even, by_odd)] + [
        a - b for a, b in zip(by_even[::-1], by_odd[::-1])
    ]


def stiff_line(values, factors):
    return derive_back([g * d for g, d in zip(factors, derive(values))])


def lanes_of(value, index):
    return jnp.take_along_axis(value, index, axis=1, mode="promise_in_bounds")


class Shared:
    def __init__(self):
        lane = lax.broadcasted_iota(jnp.int32, (8, 128), 1)
        row = lax.broadcasted_iota(jnp.int32, (8, 128), 0)
        pos_z = lane % EL_Z
        up = lane - pos_z + (pos_z + 1) % EL_Z
        down = lane - pos_z + (pos_z + EL_Z - 1) % EL_Z
        self.across = jnp.where(row == 0, up, down)
        self.has_low = lane >= EL_Z
        self.has_high = lane < CELLS - EL_Z
        self.first = row == 0
        self.last = row == NODES - 1
        self.front = pos_z == 0
        self.back = pos_z == EL_Z - 1

    def plane(self, rows):
        low, high = rows[0], rows[-1]
        zero = jnp.zeros_like(low)
        new_low = low + jnp.where(self.has_low, pltpu.roll(high, EL_Z, 1), zero)
        new_high = high + jnp.where(self.has_high, pltpu.roll(low, CELLS - EL_Z, 1), zero)
        out = []
        for value in [new_low, *rows[1:-1], new_high]:
            moved = lanes_of(value, self.across)
            from_last = pltpu.roll(moved, 1, 0)
            from_first = pltpu.roll(moved, NODES - 1, 0)
            added = jnp.where(self.first, from_last, jnp.where(self.last, from_first, zero))
            out.append(value + added)
        return out


def share(shared, ref, a, rows):
    low, high = rows[0], rows[-1]
    zero = jnp.zeros_like(low)
    new_low = low + jnp.where(shared.has_low, pltpu.roll(high, EL_Z, 1), zero)
    new_high = high + jnp.where(shared.has_high, pltpu.roll(low, CELLS - EL_Z, 1), zero)
    put_rows(ref, [new_low, *rows[1:-1], new_high], a)
    near, far = pl.ds(0, NODES, stride=8), pl.ds(NODES - 1, NODES, stride=8)
    first, last = ref[a, near, :], ref[a, far, :]
    before = jnp.where(shared.front, pltpu.roll(last, CELLS - EL_Z + 1, 1), pltpu.roll(last, 1, 1))
    after = jnp.where(shared.back, pltpu.roll(first, EL_Z - 1, 1), pltpu.roll(first, CELLS - 1, 1))
    ref[a, near, :] = first + before
    ref[a, far, :] = last + after


def rows_of(ref, *at):
    return [ref[(*at, pl.ds(8 * b, 8), slice(None))] for b in range(NODES)]


def put_rows(ref, values, *at):
    for b, value in enumerate(values):
        ref[(*at, pl.ds(8 * b, 8), slice(None))] = value


def turned(ref, *at):
    return [ref[(*at, pl.ds(c, 8, stride=8), slice(None))] for c in range(NODES)]


def mirrored():
    core = lax.axis_index("core")
    return [a + core * (NODES - 1 - 2 * a) for a in range(NODES)]


def prepare(order_in, load_in, geom_in, mass_in, load, geo_a, geo_b, geo_c, mass, diag, lead, message, order_ref, raw, work, index_ref, sems):
    order_copy = pltpu.make_async_copy(order_in, order_ref, sems.at[5])
    order_copy.start()
    sources = [geom_in.at[0], geom_in.at[1], geom_in.at[2], mass_in, load_in]
    copies = [pltpu.make_async_copy(src, raw.at[i], sems.at[i]) for i, src in enumerate(sources)]
    for copy in copies:
        copy.start()

    @pl.when(lax.axis_index("core") >= 0)
    def invert():
        order_copy.wait()
        cells = jnp.broadcast_to(order_ref[...], (CELLS, CELLS))
        hot = (cells == lax.broadcasted_iota(jnp.int32, (CELLS, CELLS), 0)).astype(F32)
        column = lax.broadcasted_iota(jnp.int32, (8, CELLS), 1).astype(F32)
        index = lax.dot_general(column, hot, (((1,), (1,)), ((), ())), preferred_element_type=F32)
        index_ref[...] = index.astype(jnp.int32)

    at = mirrored()
    for copy in copies[:3]:
        copy.wait()
    index = index_ref[...]

    def fetch(which, a):
        return [lanes_of(v, index) for v in rows_of(raw, which, at[a])]

    for b in range(NODES):
        here = pl.ds(8 * b, 8)
        lines = [lanes_of(raw[0, at[a], here, :], index) for a in range(NODES)]
        part = square_back(lines)
        for a in range(NODES):
            geo_a[a, here, :] = lines[a]
        lead[here, :] = part[0]
        for a in range(1, NODES - 1):
            diag[a, here, :] = part[a]
        message[1, here, :] = part[NODES - 1]
    for a in range(NODES):
        lines = [lanes_of(v, index) for v in turned(raw, 2, at[a])]
        put_rows(geo_c, lines, a)
        if 0 < a < NODES - 1:
            put_rows(work, square_back(lines), a)
        elif a == NODES - 1:
            put_rows(message, lines, 4)
    for copy in copies[3:]:
        copy.wait()
    for a in range(NODES):
        lines, weights, values = fetch(1, a), fetch(3, a), fetch(4, a)
        put_rows(geo_b, lines, a)
        put_rows(mass, weights, a)
        put_rows(load, values, a)
        if a == 0:
            put_rows(lead, [x + y for x, y in zip(rows_of(lead), weights)])
        elif a == NODES - 1:
            for i, rows in ((0, values), (2, weights), (3, lines)):
                put_rows(message, rows, i)
        else:
            parts = square_back(lines), turned(work, a), weights, rows_of(diag, a)
            put_rows(diag, [w + x + y + z for w, x, y, z in zip(*parts)], a)


def summed(ref, which):
    return [x + y for x, y in zip(rows_of(ref, 0, which), rows_of(ref, 1, which))]


def settle(shared, load, lead, fac_b, fac_c, work):
    put_rows(work, square_back(fac_c))
    low = [x + y + z for x, y, z in zip(square_back(fac_b), turned(work), lead)]
    low = [1.0 / v for v in shared.plane(low)]
    top = shared.plane(load)
    return top, low, [x * y * F32(1.0 / CENTRE) for x, y in zip(top, low)]


def within(values, lead, fac_b, fac_c, keep, work):
    put_rows(keep, values)
    put_rows(work, stiff_line(turned(keep), fac_c))
    part = stiff_line(values, fac_b)
    return [k * u + x + y for k, u, x, y in zip(lead, values, part, turned(work))]


def begin(load, geo_a, geo_b, geo_c, diag, lead, pair, start, recip, first, slope, message, end, keep, work):
    shared = Shared()
    mass_7, fac_b, fac_c = summed(pair, 2), summed(pair, 3), summed(pair, 4)
    lead_7 = [x + y for x, y in zip(summed(pair, 1), mass_7)]
    top, low, tail = settle(shared, summed(pair, 0), lead_7, fac_b, fac_c, work)
    put_rows(start, top, NODES - 1)
    put_rows(recip, low, NODES - 1)
    put_rows(first, tail, NODES - 1)
    put_rows(end, lead_7, 0)
    put_rows(end, fac_b, 1)
    put_rows(end, fac_c, 2)
    put_rows(end, mass_7, 3)
    for a in range(1, NODES - 1):
        share(shared, start, a, rows_of(load, a))
        share(shared, recip, a, rows_of(diag, a))
    for a in range(1, NODES - 1):
        top, low = rows_of(start, a), [1.0 / v for v in rows_of(recip, a)]
        put_rows(recip, low, a)
        put_rows(first, [x * y * F32(1.0 / CENTRE) for x, y in zip(top, low)], a)
    for b in range(NODES):
        here = pl.ds(8 * b, 8)
        zero = jnp.zeros((8, 128), F32)
        grad = derive([zero] + [first[a, here, :] for a in range(1, NODES)])
        for a in range(NODES):
            slope[a, here, :] = grad[a]
        flux = [geo_a[a, here, :] * grad[a] for a in range(NODES)]
        message[1, here, :] = combine(DERIV[:, 0], flux)
    put_rows(message, rows_of(load, 0), 0)
    put_rows(message, rows_of(lead), 2)
    put_rows(message, rows_of(geo_b, 0), 3)
    put_rows(message, rows_of(geo_c, 0), 4)

    @pl.when(lax.axis_index("core") == 0)
    def inner():
        tail = rows_of(first, NODES - 1)
        put_rows(end, within(tail, rows_of(end, 3), rows_of(end, 1), rows_of(end, 2), keep, work), 3)


def improve(first, image, recip):
    return [u * F32(KEEP) + q * d * F32(PULL) for u, q, d in zip(first, image, recip)]


def middle(both, end, geo_a, geo_b, geo_c, mass, recip, first, slope, start0, precond, ahead, message, keep, local, work):
    shared = Shared()
    once = (1 - lax.axis_index("core")).astype(F32)
    lead, fac_b, fac_c = summed(both, 2), summed(both, 3), summed(both, 4)
    top, low, head = settle(shared, summed(both, 0), lead, fac_b, fac_c, work.at[0])
    put_rows(start0, top)
    image = within(head, lead, fac_b, fac_c, keep, work.at[0])
    image = shared.plane([x + y for x, y in zip(summed(both, 1), image)])
    put_rows(precond, improve(head, image, low), 0)
    for b in range(NODES):
        here = pl.ds(8 * b, 8)
        flux = []
        for a in range(NODES):
            flux.append(geo_a[a, here, :] * (slope[a, here, :] + head[b] * F32(DERIV[a, 0])))
        back = derive_back(flux)
        for a in range(1, NODES - 1):
            local[a, here, :] = back[a]
        message[0, here, :] = back[NODES - 1] + end[3, here, :] * once
    for a in range(1, NODES - 1):
        put_rows(work, stiff_line(turned(first, a), rows_of(geo_c, a)), a)
    for a in range(1, NODES - 1):
        values = rows_of(first, a)
        part = stiff_line(values, rows_of(geo_b, a))
        turn = turned(work, a)
        image = [
            x + y + z + m * v
            for x, y, z, m, v in zip(rows_of(local, a), part, turn, rows_of(mass, a), values)
        ]
        put_rows(precond, improve(values, shared.plane(image), rows_of(recip, a)), a)
    for b in range(NODES):
        here = pl.ds(8 * b, 8)
        zero = jnp.zeros((8, 128), F32)
        grad = derive([precond[a, here, :] for a in range(NODES - 1)] + [zero])
        for a in range(NODES):
            ahead[a, here, :] = grad[a]
        flux = [geo_a[a, here, :] * grad[a] for a in range(NODES)]
        message[1, here, :] = combine(DERIV[:, NODES - 1], flux)


def finish(pair, end, geo_a, geo_b, geo_c, mass, load, recip, first, precond_in, ahead, precond, image, outer, row, keep, flux_a, flux_b, flux_c, row_buf, row_sem):
    shared = Shared()
    whole = shared.plane(summed(pair, 0))
    tail = improve(rows_of(first, NODES - 1), whole, rows_of(recip, NODES - 1))
    put_rows(precond, tail)

    def iterate(a):
        return tail if a == NODES - 1 else rows_of(precond_in, a)

    over = [jnp.zeros((8, 128), F32) for _ in range(NODES)]
    under = [jnp.zeros((8, 128), F32) for _ in range(NODES)]
    for b in range(NODES):
        here = pl.ds(8 * b, 8)
        for a in range(NODES):
            grad = ahead[a, here, :] + tail[b] * F32(DERIV[a, NODES - 1])
            flux = geo_a[a, here, :] * grad
            flux_a[a, here, :] = flux
            under[a] = under[a] + flux * grad
    for a in range(NODES):
        grad = derive(turned(precond) if a == NODES - 1 else turned(precond_in, a))
        flux = [g * d for g, d in zip(rows_of(geo_c, a), grad)]
        put_rows(flux_c, flux, a)
        under = [s + f * d for s, f, d in zip(under, flux, grad)]
    for a in range(NODES):
        values = iterate(a)
        grad = derive(values)
        flux = [g * d for g, d in zip(rows_of(geo_b, a), grad)]
        put_rows(flux_b, flux, a)
        under = [s + f * d for s, f, d in zip(under, flux, grad)]
        under = [s + m * v * v for s, m, v in zip(under, rows_of(mass, a), values)]
        over = [s + f * v for s, f, v in zip(over, rows_of(load, a), values)]
    over = jnp.sum(functools.reduce(jnp.add, over), axis=0, keepdims=True)
    under = jnp.sum(functools.reduce(jnp.add, under), axis=0, keepdims=True)
    over = over + pltpu.roll(over, 64, 1)
    under = under + pltpu.roll(under, 64, 1)
    lane = lax.broadcasted_iota(jnp.int32, (1, 128), 1)
    row_buf[...] = jnp.broadcast_to(jnp.where(lane < 64, over, under), row_buf.shape)
    row_copy = pltpu.make_async_copy(row_buf, row, row_sem)
    row_copy.start()

    @pl.when(lax.axis_index("core") >= 0)
    def apply():
        for b in range(NODES):
            here = pl.ds(8 * b, 8)
            back = derive_back([flux_a[a, here, :] for a in range(NODES)])
            for a in range(NODES - 1):
                flux_a[a, here, :] = back[a]
        for a in range(NODES - 1):
            put_rows(flux_c, derive_back(rows_of(flux_c, a)), a)
        for a in range(NODES - 1):
            values = rows_of(precond_in, a)
            part = derive_back(rows_of(flux_b, a))
            turn = turned(flux_c, a)
            total = [
                x + y + z + m * v
                for x, y, z, m, v in zip(rows_of(flux_a, a), part, turn, rows_of(mass, a), values)
            ]
            if a == 0:
                put_rows(outer, Shared().plane(total))
            else:
                put_rows(image, Shared().plane(total), a)
        inside = within(rows_of(precond), rows_of(end, 0), rows_of(end, 1), rows_of(end, 2), keep, flux_c.at[NODES - 1])
        inside = [x + y for x, y in zip(summed(pair, 1), inside)]
        put_rows(image, Shared().plane(inside), NODES - 1)

    row_copy.wait()


def restore(order_ref, start_in, start0, precond_in, last, image_in, outer, start, precond, image):
    index = jnp.broadcast_to(order_ref[...], (8, CELLS))
    for a in range(NODES):
        for out, rows in (
            (start, rows_of(start0) if a == 0 else rows_of(start_in, a)),
            (precond, rows_of(last) if a == NODES - 1 else rows_of(precond_in, a)),
            (image, rows_of(outer) if a == 0 else rows_of(image_in, a)),
        ):
            put_rows(out, [lanes_of(v, index) for v in rows], a)


def step_length(sums, alpha):
    lane = lax.broadcasted_iota(jnp.int32, (1, 128), 1)
    total = jnp.sum(sums[...], axis=0, keepdims=True)
    zero = jnp.zeros_like(total)
    over = jnp.sum(jnp.where(lane < 64, total, zero), axis=1, keepdims=True)
    under = jnp.sum(jnp.where(lane < 64, zero, total), axis=1, keepdims=True)
    alpha[...] = jnp.broadcast_to(over / under, (8, 128))


def close(alpha_ref, order_ref, other, start, precond, image, solution_out, residual_out, buf_s, buf_r, sems):
    alpha = alpha_ref[...]
    index = jnp.broadcast_to(order_ref[...], (8, CELLS))
    at = mirrored()
    other = [lanes_of(v, index) for v in rows_of(other)]
    copies = []

    def send(i, a):
        buf, out = ((buf_s, solution_out), (buf_r, residual_out))[i]
        copies.append(pltpu.make_async_copy(buf.at[a], out.at[at[a]], sems.at[i, a]))
        copies[-1].start()

    for a in (1, 2, 3, 4, 5, 6, 7, 0):
        for b, v in enumerate(rows_of(precond, a)):
            buf_s[a, b] = alpha * v
        send(0, a)
        rows = rows_of(image, a)
        if a == 0:
            rows = [x + y for x, y in zip(rows, other)]
        for b, (s, i) in enumerate(zip(rows_of(start, a), rows)):
            buf_r[a, b] = s - alpha * i
        send(1, a)
    for copy in copies:
        copy.wait()


def gather_up(sums, row):
    row[...] = jnp.broadcast_to(jnp.sum(sums[...], axis=0, keepdims=True), row.shape)


VMEM = pl.BlockSpec(memory_space=pltpu.VMEM)
HBM = pl.BlockSpec(memory_space=pltpu.HBM)
ANY = pl.BlockSpec(memory_space=pl.ANY)
FIELD = (NODES, 64, 128)
FACE = (64, 128)
BLOCK = (NODES, NODES, NODES, CELLS)


def call(body, outs, ins, scratch=(), out_specs=None, flops=4_000_000):
    return pl.pallas_call(
        body,
        out_shape=[jax.ShapeDtypeStruct(s, F32) if isinstance(s, tuple) else s for s in outs],
        in_specs=ins,
        out_specs=out_specs or [VMEM] * len(outs),
        scratch_shapes=list(scratch),
        compiler_params=pltpu.CompilerParams(vmem_limit_bytes=12 << 20),
        cost_estimate=pl.CostEstimate(flops=flops, bytes_accessed=2 << 20, transcendentals=0),
    )


def on_device(load_terms, geometry, mass_terms, element_order):
    count = 1
    for axis in AXES:
        count *= lax.axis_size(axis)
    across_chips = [[2 * k + 1, (2 * k + 2) % count] for k in range(count // 2)]
    first_groups, second_groups = groups((1, 3)), groups((0, 2))
    in_chip = [[2 * k + 1, 2 * k] for k in range(count // 2)]
    swap = [(i, (i + 1) % count if i % 2 else (i - 1) % count) for i in range(count)]
    dma = pltpu.SemaphoreType.DMA
    arguments = (
        element_order,
        load_terms.reshape(FIELD),
        geometry.reshape(3, *FIELD),
        mass_terms.reshape(FIELD),
    )
    arguments = [pltpu.with_memory_space_constraint(x, pltpu.HBM) for x in arguments]

    load, geo_a, geo_b, geo_c, mass, diag, lead, message, order = call(
        prepare,
        [FIELD] * 6 + [FACE, (5, *FACE), jax.ShapeDtypeStruct((1, CELLS), jnp.int32)],
        [HBM] * 4,
        [
            pltpu.VMEM((5, *FIELD), F32),
            pltpu.VMEM(FIELD, F32),
            pltpu.VMEM((8, CELLS), jnp.int32),
            dma((6,)),
        ],
    )(*arguments)
    pair = lax.all_gather(message, AXES, axis_index_groups=in_chip)
    start, recip, first, slope, message, end = call(
        begin, [FIELD] * 4 + [(5, *FACE), (4, *FACE)], [VMEM] * 7, [pltpu.VMEM(FACE, F32), pltpu.VMEM(FACE, F32)]
    )(load, geo_a, geo_b, geo_c, diag, lead, pair)
    both = lax.all_gather(message, AXES, axis_index_groups=across_chips)
    start0, precond, ahead, message = call(
        middle,
        [FACE, FIELD, FIELD, (2, *FACE)],
        [VMEM] * 9,
        [pltpu.VMEM(FACE, F32), pltpu.VMEM(FIELD, F32), pltpu.VMEM(FIELD, F32)],
    )(both, end, geo_a, geo_b, geo_c, mass, recip, first, slope)
    pair = lax.all_gather(message, AXES, axis_index_groups=in_chip)
    last, image, outer, row = call(
        finish,
        [FACE, FIELD, FACE, (len(first_groups[0]), 128)],
        [VMEM] * 11,
        [
            pltpu.VMEM(FACE, F32),
            *[pltpu.VMEM(FIELD, F32)] * 3,
            pltpu.VMEM((len(first_groups[0]), 128), F32),
            dma,
        ],
        out_specs=[VMEM] * 3 + [ANY],
    )(pair, end, geo_a, geo_b, geo_c, mass, load, recip, first, precond, ahead)
    outer_other = lax.ppermute(outer, AXES, swap)
    sums = lax.all_to_all(row, AXES, 0, 0, tiled=True, axis_index_groups=first_groups)
    (row,) = call(gather_up, [(len(second_groups[0]), 128)], [VMEM], flops=100_000)(sums)
    sums = lax.all_to_all(row, AXES, 0, 0, tiled=True, axis_index_groups=second_groups)
    (alpha,) = call(step_length, [(8, 128)], [VMEM], flops=100_000)(sums)
    start, precond, image = call(restore, [FIELD] * 3, [VMEM] * 7)(order, start, start0, precond, last, image, outer)
    solution, residual = call(
        close,
        [BLOCK, BLOCK],
        [VMEM] * 6,
        [pltpu.VMEM(BLOCK, F32), pltpu.VMEM(BLOCK, F32), dma((2, NODES))],
        out_specs=[ANY, ANY],
    )(alpha, order, outer_other, start, precond, image)
    return solution, residual


def solution(mesh):
    torus = Mesh(mesh.devices.reshape(TORUS), AXES)
    placed = (
        P(None, None, None, AXES),
        P(None, None, None, None, AXES),
        P(None, None, None, AXES),
        P(AXES, None),
    )
    return jax.shard_map(
        on_device,
        mesh=torus,
        in_specs=placed,
        out_specs=(P(None, None, None, AXES), P(None, None, None, AXES)),
        check_vma=False,
    )
```
